32 devices in a mesh: rows: 8 (over z, y), feat: 4 (over x, core).
Axes of the slice: x: 2, y: 2, z: 4, core: 2. Of those that a mesh axis runs over, the one named last changes fastest.
Arguments:
- cells: bfloat16 [1024, 80, 128], P('rows', 'feat'), may hold values from -19 to 19
- block_table: int32 [8], replicated, may hold values from 0 to 7, as said below
- row_live: int32 [1024], replicated, may hold values from 0 to 1, as said below
- row_train: int32 [1024], replicated, may hold values from 0 to 1, as said below
- feat_qkv: bfloat16 [128, 384], replicated, may hold values from -0.5 to 0.5
- feat_out: bfloat16 [128, 128], replicated, may hold values from -0.5 to 0.5
- item_qkv: bfloat16 [128, 384], replicated, may hold values from -0.5 to 0.5
- item_out: bfloat16 [128, 128], replicated, may hold values from -0.5 to 0.5
Outputs:
- layer_output: bfloat16 [1024, 80, 128], P(('rows', 'feat'))
The draws below stay inside these ranges and needn't reach their ends.
Inputs may be any that keep to these rules, and one draw needn't show every extreme that they name: `block_table`: every table number appears in some block. `row_live`: every training row is live. `row_train`: each aligned group of 32 rows holds 1 to 4 training rows; some group holds exactly 4.
All inputs are finite; a program needn't handle non-finite values.
Results may differ from the reference program's by a relative error of at most 0.014.
Values may be sent and summed in bfloat16 or wider, within the bound.
No kernel may reach another device: no remote copies, remote signals or barrier semaphores. Data moves between devices by JAX's collectives and lax.ppermute only.
A program may use at most 64 MiB of HBM per device.

```python
import jax
import jax.numpy as jnp
from jax import lax

F = 80
E = 128
HEADS = 4
HEAD_DIM = 32
BLOCK = 128
KEEP = 4
TABLES = 8
GROUP = 32
BLOCKS = 8
ROWS = 1024


def draw_cells(key, part):
    first_key, second_key, third_key, fourth_key = jax.random.split(jax.random.fold_in(key, 5), 4)
    base_part = jnp.clip(jax.random.normal(first_key, (ROWS, F, E), jnp.float32), -4.0, 4.0)
    log_scale = jax.random.uniform(second_key, (F,), jnp.float32, jnp.log(0.5), jnp.log(4.0))
    offsets = jax.random.uniform(third_key, (F,), jnp.float32, -2.0, 2.0)
    block_shift = 0.5 * jnp.clip(jax.random.normal(fourth_key, (ROWS // BLOCK, F, 1), jnp.float32), -2.0, 2.0)
    block_shift = jnp.repeat(block_shift, BLOCK, axis=0)
    cells_value = base_part * jnp.exp(log_scale)[None, :, None] + offsets[None, :, None] + block_shift
    return cells_value.astype(jnp.bfloat16)


def draw_block_table(key, part):
    count_blocks = ROWS // BLOCK
    first_key, second_key, third_key = jax.random.split(jax.random.fold_in(key, 3), 3)
    extra_count = count_blocks - TABLES
    low_pick = jnp.minimum(jax.random.randint(first_key, (extra_count,), 0, TABLES), jax.random.randint(second_key, (extra_count,), 0, TABLES))
    tables_all = jnp.concatenate([jnp.arange(TABLES, dtype=jnp.int32), low_pick.astype(jnp.int32)])
    return jax.random.permutation(third_key, tables_all).astype(jnp.int32)


def train_pattern(key):
    count_key, order_key = jax.random.split(jax.random.fold_in(key, 17))
    group_count = ROWS // GROUP
    counts = jax.random.randint(count_key, (group_count,), 1, KEEP + 1).astype(jnp.int32).at[0].set(KEEP)
    scores = jax.random.randint(order_key, (group_count, GROUP), 0, 1 << 20).astype(jnp.int32) * GROUP + jnp.arange(GROUP, dtype=jnp.int32)[None, :]
    ranks = jnp.argsort(jnp.argsort(scores, axis=1, stable=True), axis=1, stable=True)
    return (ranks < counts[:, None]).astype(jnp.int32).reshape(ROWS)


def draw_row_train(key, part):
    return train_pattern(key)


def draw_row_live(key, part):
    train_rows = train_pattern(key)
    chance = jax.random.randint(jax.random.fold_in(key, 29), (ROWS,), 0, 8)
    return jnp.maximum(train_rows, (chance < 7).astype(jnp.int32))


def bell_draw(key, dims, scale, bound, held_as=jnp.bfloat16):
    drawn = jax.random.normal(key, dims, jnp.float32) * scale
    return jnp.minimum(jnp.maximum(drawn, -bound), bound).astype(held_as)


def setup_inputs(seed: int = 0) -> dict:
    key_list = jax.random.split(jax.random.key(seed), 9)
    return {
        "cells": draw_cells(jax.random.fold_in(key_list[8], 71), 0),
        "block_table": draw_block_table(jax.random.fold_in(key_list[8], 71), 0),
        "row_live": draw_row_live(jax.random.fold_in(key_list[8], 71), 0),
        "row_train": draw_row_train(jax.random.fold_in(key_list[8], 71), 0),
        "feat_qkv": bell_draw(key_list[4], (E, 3 * E), E ** -0.5, 0.5),
        "feat_out": bell_draw(key_list[5], (E, E), E ** -0.5, 0.5),
        "item_qkv": bell_draw(key_list[6], (E, 3 * E), E ** -0.5, 0.5),
        "item_out": bell_draw(key_list[7], (E, E), E ** -0.5, 0.5),
    }


EPSILON = 1e-05
MASKED = -1e+30

def compact_train(train_rows):
    positions = jnp.arange(train_rows.shape[-1], dtype=jnp.int32)
    ordinal = (jnp.cumsum(train_rows, axis=-1) - 1).astype(jnp.int32)
    slot_ids = jnp.arange(KEEP, dtype=jnp.int32)
    matched = (train_rows[..., None, :] == 1) & (ordinal[..., None, :] == slot_ids[:, None])
    return lax.optimization_barrier(jnp.sum(jnp.where(matched, positions, 0), axis=-1)).astype(jnp.int32)

def feature_block(normed_block, feat_qkv, feat_out):
    row_count, feat_count, width_all = normed_block.shape
    projected = jnp.dot(normed_block, feat_qkv, preferred_element_type=jnp.float32).astype(jnp.bfloat16)
    head_shape = (row_count, feat_count, HEADS, HEAD_DIM)
    queries = projected[..., :width_all].reshape(head_shape).astype(jnp.float32)
    key_part = projected[..., width_all:2 * width_all].reshape(head_shape).astype(jnp.float32)
    value_part = projected[..., 2 * width_all:].reshape(head_shape).astype(jnp.float32)
    scores = jnp.einsum('rqhd,rkhd->rhqk', queries, key_part) * HEAD_DIM ** (-0.5)
    shares = jax.nn.softmax(scores, axis=-1).astype(jnp.bfloat16)
    attended = jnp.einsum('rhqk,rkhd->rqhd', shares.astype(jnp.float32), value_part).astype(jnp.bfloat16)
    attended = attended.reshape(row_count, feat_count, width_all)
    update = jnp.dot(attended, feat_out, preferred_element_type=jnp.float32)
    return (normed_block.astype(jnp.float32) + update).astype(jnp.bfloat16)

def reference(cells, block_table, row_live, row_train, feat_qkv, feat_out, item_qkv, item_out):
    row_table = jnp.repeat(block_table, BLOCK).astype(jnp.int32)
    table_ids = jnp.arange(TABLES, dtype=jnp.int32)
    table_hot = ((row_table[:, None] == table_ids[None, :]) & (row_live[:, None] == 1)).astype(jnp.float32)
    values = cells.astype(jnp.float32)
    count_sum = lax.optimization_barrier(jnp.sum(table_hot, axis=0)) * E
    first_sum = jnp.dot(table_hot.T, lax.optimization_barrier(jnp.sum(values, axis=2)), precision=lax.Precision.HIGHEST)
    table_mean = first_sum / count_sum[:, None]
    centred = values - table_mean[row_table][:, :, None]
    second_sum = jnp.dot(table_hot.T, lax.optimization_barrier(jnp.sum(centred * centred, axis=2)), precision=lax.Precision.HIGHEST)
    table_spread = second_sum / count_sum[:, None]
    normed = (centred * lax.rsqrt(table_spread[row_table] + EPSILON)[:, :, None]).astype(jnp.bfloat16)
    blocked = normed.reshape(BLOCKS, BLOCK, F, E)
    mixed_cells = lax.map(lambda block_cells: feature_block(block_cells, feat_qkv, feat_out), blocked)
    mixed_cells = mixed_cells.reshape(ROWS, F, E)
    group_count = ROWS // GROUP
    train_groups = row_train.reshape(group_count, GROUP)
    places = compact_train(train_groups)
    slot_ids = jnp.arange(KEEP, dtype=jnp.int32)
    key_valid = (slot_ids[None, :] < lax.optimization_barrier(jnp.sum(train_groups, axis=1)).astype(jnp.int32)[:, None]).reshape(-1)
    key_rows = (jnp.arange(group_count, dtype=jnp.int32)[:, None] * GROUP + places).reshape(-1)
    key_table = row_table[key_rows]
    chosen = mixed_cells[key_rows]
    queries = jnp.dot(mixed_cells, item_qkv[:, :E], preferred_element_type=jnp.float32).astype(jnp.bfloat16)
    key_value = jnp.dot(chosen, item_qkv[:, E:], preferred_element_type=jnp.float32).astype(jnp.bfloat16)
    queries = queries.reshape(ROWS, F, HEADS, HEAD_DIM)
    key_part = key_value[..., :E].reshape(-1, F, HEADS, HEAD_DIM)
    value_part = key_value[..., E:].reshape(-1, F, HEADS, HEAD_DIM)
    allowed = (row_table[:, None] == key_table[None, :]) & key_valid[None, :]

    def one_feature(feature_parts):
        feature_query, feature_key, feature_value = feature_parts
        scores = jnp.einsum('qhd,khd->hqk', feature_query.astype(jnp.float32), feature_key.astype(jnp.float32))
        scores = jnp.where(allowed[None], scores * HEAD_DIM ** (-0.5), MASKED)
        shares = jax.nn.softmax(scores, axis=-1).astype(jnp.bfloat16)
        return jnp.einsum('hqk,khd->qhd', shares.astype(jnp.float32), feature_value.astype(jnp.float32)).astype(jnp.bfloat16)
    attended = lax.map(one_feature, (jnp.moveaxis(queries, 1, 0), jnp.moveaxis(key_part, 1, 0), jnp.moveaxis(value_part, 1, 0)))
    attended = jnp.moveaxis(attended, 0, 1).reshape(ROWS, F, E)
    update = jnp.dot(attended, item_out, preferred_element_type=jnp.float32)
    return (mixed_cells.astype(jnp.float32) + update).astype(jnp.bfloat16)
```

```python
import functools
import math

import jax
import jax.numpy as jnp
from jax import lax
from jax.experimental import pallas as pl
from jax.experimental.pallas import tpu as pltpu
from jax.sharding import PartitionSpec as P

HEADS = 4
HEAD_DIM = 32
KEEP = 4
TABLES = 8


EPSILON = 1e-05
MASKED = -1e30
SCALE2 = HEAD_DIM ** (-0.5) * math.log2(math.e)


def compact_train(train_rows):
    positions = jnp.arange(train_rows.shape[-1], dtype=jnp.int32)
    ordinal = jnp.cumsum(train_rows, axis=-1) - 1
    slot_ids = jnp.arange(KEEP, dtype=jnp.int32)
    matched = (train_rows[..., None, :] == 1) & (ordinal[..., None, :] == slot_ids[:, None])
    return jnp.sum(jnp.where(matched, positions, 0), axis=-1)


def into_heads(tensor):
    return tensor.reshape(tensor.shape[:-1] + (HEADS, HEAD_DIM))


def attend_features(queries, key_part, value_part):
    row_count, query_feats = (queries.shape[0], queries.shape[1])
    blocks = max(1, row_count * query_feats // 1280)
    while row_count % blocks:
        blocks -= 1
    scaling = HEAD_DIM ** (-0.5)

    def attend_one_block(block_parts):
        block_query, block_key, block_value = block_parts
        scores = (
            jnp.einsum(
                "rqhd,rkhd->rhqk", block_query, block_key, preferred_element_type=jnp.float32
            )
            * scaling
        )
        shares = jax.nn.softmax(scores, axis=-1).astype(jnp.bfloat16)
        return jnp.einsum(
            "rhqk,rkhd->rqhd", shares, block_value, preferred_element_type=jnp.float32
        ).astype(jnp.bfloat16)

    def by_block(tensor):
        return tensor.reshape((blocks, row_count // blocks) + tensor.shape[1:])

    result = lax.map(
        attend_one_block, (by_block(queries), by_block(key_part), by_block(value_part))
    )
    return result.reshape(row_count, query_feats, HEADS * HEAD_DIM)


def feature_layer(normed_cells, feat_out, key_part, value_part, queries):
    attended = attend_features(queries, key_part, value_part)
    update = jnp.dot(attended, feat_out, preferred_element_type=jnp.float32)
    return (normed_cells.astype(jnp.float32) + update).astype(jnp.bfloat16)


def on_device(cells, block_table, row_live, row_train, feat_qkv, feat_out, item_qkv, item_out):
    rows_here, feats_here, width_all = cells.shape
    row_index = lax.axis_index("rows")
    feat_index = lax.axis_index("feat")
    row_devices = lax.axis_size("rows")
    feat_devices = lax.axis_size("feat")
    my_table = lax.dynamic_index_in_dim(block_table, row_index, keepdims=False)
    live_rows = lax.dynamic_slice_in_dim(row_live, row_index * rows_here, rows_here).astype(
        jnp.float32
    )
    values = cells.astype(jnp.float32)
    table_hot = (jnp.arange(TABLES, dtype=jnp.int32) == my_table).astype(jnp.float32)
    first_local = jnp.sum(values * live_rows[:, None, None], axis=(0, 2))
    count_local = jnp.sum(live_rows) * width_all
    first_sum, count_sum = lax.psum(
        (table_hot[:, None] * first_local[None, :], table_hot * count_local), "rows"
    )
    table_mean = first_sum / count_sum[:, None]
    mine_mean = lax.dynamic_index_in_dim(table_mean, my_table, keepdims=False)
    centred = values - mine_mean[None, :, None]
    second_local = jnp.sum(centred * centred * live_rows[:, None, None], axis=(0, 2))
    second_sum = lax.psum(table_hot[:, None] * second_local[None, :], "rows")
    table_spread = second_sum / count_sum[:, None]
    mine_spread = lax.dynamic_index_in_dim(table_spread, my_table, keepdims=False)
    normed = (centred * lax.rsqrt(mine_spread + EPSILON)[None, :, None]).astype(jnp.bfloat16)
    normed_rows = lax.all_to_all(normed, "feat", split_axis=0, concat_axis=1, tiled=True)
    projected = jnp.dot(normed_rows, feat_qkv, preferred_element_type=jnp.float32).astype(
        jnp.bfloat16
    )
    queries = into_heads(projected[..., :width_all])
    key_part = into_heads(projected[..., width_all : 2 * width_all])
    value_part = into_heads(projected[..., 2 * width_all :])
    mixed_rows = feature_layer(normed_rows, feat_out, key_part, value_part, queries)
    group_rows, total_feats = (mixed_rows.shape[0], mixed_rows.shape[1])
    per_device = total_feats * HEADS // row_devices
    first_row = row_index * rows_here + feat_index * group_rows
    train_here = lax.dynamic_slice_in_dim(row_train, first_row, group_rows)
    places = compact_train(train_here)
    chosen = jnp.take(mixed_rows, places, axis=0)
    item_query = jnp.dot(
        mixed_rows, item_qkv[:, :width_all], preferred_element_type=jnp.float32
    ).astype(jnp.bfloat16)
    item_query = item_query.reshape(group_rows, row_devices, per_device, HEAD_DIM)
    key_value = jnp.dot(chosen, item_qkv[:, width_all:], preferred_element_type=jnp.float32).astype(
        jnp.bfloat16
    )
    item_key = key_value[..., :width_all].reshape(KEEP, row_devices, per_device, HEAD_DIM)
    item_value = key_value[..., width_all:].reshape(KEEP, row_devices, per_device, HEAD_DIM)
    query_table = jnp.repeat(block_table, group_rows)
    groups_all = row_train.reshape(row_devices, feat_devices, group_rows)
    group_counts = jnp.sum(groups_all, axis=2)
    slot_ids = jnp.arange(KEEP, dtype=jnp.int32)
    key_valid = slot_ids[None, None, :] < jnp.transpose(group_counts)[:, :, None]
    key_table = jnp.broadcast_to(block_table[None, :, None], key_valid.shape)
    allowed = (query_table[:, None] == key_table.reshape(-1)[None, :]) & key_valid.reshape(-1)[
        None, :
    ]
    query_count = query_table.shape[0]
    key_count = allowed.shape[1]
    query_blocks = max(1, query_count // 512)
    while query_count % query_blocks:
        query_blocks -= 1
    scaling = HEAD_DIM ** (-0.5)
    blocked_allowed = allowed.reshape(query_blocks, query_count // query_blocks, key_count)
    local_query = lax.all_to_all(item_query, "rows", split_axis=1, concat_axis=0, tiled=True)
    local_key = lax.all_to_all(item_key, "rows", split_axis=1, concat_axis=0, tiled=True)
    local_value = lax.all_to_all(item_value, "rows", split_axis=1, concat_axis=0, tiled=True)
    every_key = lax.all_gather(local_key, "feat", axis=0, tiled=True)
    every_value = lax.all_gather(local_value, "feat", axis=0, tiled=True)

    def one_item(item_parts):
        single_query, single_key, single_value = item_parts

        def one_one_block(block_parts):
            block_query, block_allowed = block_parts
            scores = (
                jnp.dot(block_query, single_key.T, preferred_element_type=jnp.float32) * scaling
            )
            scores = jnp.where(block_allowed, scores, MASKED)
            shares = jax.nn.softmax(scores, axis=-1).astype(jnp.bfloat16)
            return jnp.dot(shares, single_value, preferred_element_type=jnp.float32).astype(
                jnp.bfloat16
            )

        blocked_query = single_query.reshape(query_blocks, query_count // query_blocks, HEAD_DIM)
        return lax.map(one_one_block, (blocked_query, blocked_allowed)).reshape(
            query_count, HEAD_DIM
        )

    by_item = (
        jnp.moveaxis(local_query[:, 0], 1, 0),
        jnp.moveaxis(every_key[:, 0], 1, 0),
        jnp.moveaxis(every_value[:, 0], 1, 0),
    )
    result = jnp.moveaxis(lax.map(one_item, by_item), 0, 1)[:, None]
    attended = lax.all_to_all(result, "rows", split_axis=0, concat_axis=1, tiled=True)
    attended = attended.reshape(group_rows, total_feats, width_all)
    update = jnp.dot(attended, item_out, preferred_element_type=jnp.float32)
    return (mixed_rows.astype(jnp.float32) + update).astype(jnp.bfloat16)


def prepare_kernel(chunks, live_ref, train_ref, cells_ref, bias_ref, train_out, *refs):
    place = refs[-1]
    outs = refs[:-1]
    rows_here, feats_here, width = cells_ref.shape
    feat_devices = lax.axis_size("feat")
    group_rows = rows_here // feat_devices
    feat_index = lax.axis_index("feat")
    base = lax.axis_index("rows") * rows_here

    def first(step, carry):
        total, count = carry
        for inner in range(8):
            row = step * 8 + inner
            weight = live_ref[base + row].astype(jnp.float32)
            total = total + cells_ref[row].astype(jnp.float32) * weight
            count = count + weight
        return total, count

    zeros = jnp.zeros((feats_here, width), jnp.float32)
    total, count = lax.fori_loop(0, rows_here // 8, first, (zeros, jnp.float32(0)))
    entries = jnp.full((feats_here, 1), count * width, jnp.float32)
    mean = jnp.broadcast_to(jnp.sum(total, axis=1, keepdims=True) / entries, (feats_here, width))

    def second(step, total):
        for inner in range(8):
            row = step * 8 + inner
            weight = live_ref[base + row].astype(jnp.float32)
            centred = cells_ref[row].astype(jnp.float32) - mean
            total = total + centred * centred * weight
        return total

    total = lax.fori_loop(0, rows_here // 8, second, zeros)
    spread = jnp.sum(total, axis=1, keepdims=True) / entries
    factor = jnp.broadcast_to(lax.rsqrt(spread + EPSILON), (feats_here, width))

    def normed(row):
        return ((cells_ref[row].astype(jnp.float32) - mean) * factor).astype(jnp.bfloat16)

    lane = lax.broadcasted_iota(jnp.int32, bias_ref.shape, 1)
    counts = jnp.zeros(bias_ref.shape, jnp.int32)
    for group in range(feat_devices):
        for slot in range(KEEP):
            place[group * (KEEP + 1) + slot] = group * group_rows

        def scan(row, count):
            place[group * (KEEP + 1) + count] = group * group_rows + row
            return count + train_ref[base + group * group_rows + row]

        found = lax.fori_loop(0, group_rows, scan, jnp.int32(0), unroll=True)
        counts = jnp.where(lane // KEEP == group, found, counts)
    bias_ref[...] = jnp.where(lane % KEEP < counts, 0.0, MASKED)

    for group in range(feat_devices):
        for slot in range(KEEP):
            key = group * KEEP + slot
            train_out[pl.ds(key * feats_here, feats_here), :] = normed(
                place[group * (KEEP + 1) + slot]
            )
    for step in range(feat_devices):
        first_row = (feat_index ^ step) * group_rows
        done = 0
        for at, size in enumerate(chunks):
            out = outs[step * len(chunks) + at]
            for row in range(size):
                out[pl.ds(row * feats_here, feats_here), :] = normed(first_row + done + row)
            done += size


def prepare(cells, row_live, row_train, chunks):
    rows_here, feats_here, width = cells.shape
    feat_devices = lax.axis_size("feat")
    keys = feat_devices * KEEP
    shapes = [
        jax.ShapeDtypeStruct((8, 128), jnp.float32),
        jax.ShapeDtypeStruct((keys * feats_here, width), jnp.bfloat16),
    ]
    for _ in range(feat_devices):
        for size in chunks:
            shapes.append(jax.ShapeDtypeStruct((size * feats_here, width), jnp.bfloat16))
    outs = pl.pallas_call(
        functools.partial(prepare_kernel, chunks),
        out_shape=shapes,
        in_specs=[
            pl.BlockSpec(memory_space=pltpu.SMEM),
            pl.BlockSpec(memory_space=pltpu.SMEM),
            pl.BlockSpec(memory_space=pltpu.VMEM),
        ],
        out_specs=[pl.BlockSpec(memory_space=pltpu.VMEM)] * len(shapes),
        scratch_shapes=[pltpu.SMEM((feat_devices * (KEEP + 1),), jnp.int32)],
        name="prepare",
    )(row_live, row_train, cells)
    bias, train_rows = outs[0], outs[1]
    sends = [
        [outs[2 + step * len(chunks) + at] for at in range(len(chunks))]
        for step in range(feat_devices)
    ]
    return bias, train_rows, sends


def assemble(parts, held, joined, rows):
    feat_devices = len(parts)
    feats_here = parts[0].shape[0] // rows
    total_feats = feat_devices * feats_here
    feat_index = lax.axis_index("feat")
    for step in range(feat_devices):
        held[feat_index ^ step] = parts[step][...]
    for row in range(rows):
        for source in range(feat_devices):
            joined[pl.ds(row * total_feats + source * feats_here, feats_here), :] = held[
                source, pl.ds(row * feats_here, feats_here), :
            ]


def head_masks(rows, width):
    lane = lax.broadcasted_iota(jnp.int32, (rows, width), 1)
    return [(lane // HEAD_DIM) == head for head in range(HEADS)]


def attend(queries, keys, values, masks, bias):
    count, width = queries.shape
    stacked = jnp.concatenate(
        [jnp.where(mask, queries, jnp.zeros_like(queries)) for mask in masks[0]], axis=0
    )
    scores = lax.dot_general(
        stacked, keys, (((1,), (1,)), ((), ())), preferred_element_type=jnp.float32
    )
    if bias is not None:
        scores = scores + bias
    top = jnp.max(scores, axis=1, keepdims=True)
    shares = jnp.exp2((scores - top) * SCALE2).astype(jnp.bfloat16)
    both = jnp.concatenate([values, jnp.ones_like(values)], axis=1)
    mixed = jnp.dot(shares, both, preferred_element_type=jnp.float32)
    out, total = mixed[:count, :width], mixed[:count, width:]
    for head in range(1, HEADS):
        block = mixed[head * count : (head + 1) * count]
        out = jnp.where(masks[1][head], block[:, :width], out)
        total = jnp.where(masks[1][head], block[:, width:], total)
    return out / total


def feature_rows(joined, base, rows, feats, qkv_ref, out_ref):
    width = joined.shape[1]
    cells = joined[pl.ds(base, rows * feats), :]
    projected = jnp.dot(cells, qkv_ref[...], preferred_element_type=jnp.float32).astype(
        jnp.bfloat16
    )
    masks = head_masks(feats, width)
    attended = []
    for row in range(rows):
        block = projected[row * feats : (row + 1) * feats]
        attended.append(
            attend(
                block[:, :width],
                block[:, width : 2 * width],
                block[:, 2 * width :],
                (masks, masks),
                None,
            ).astype(jnp.bfloat16)
        )
    attended = jnp.concatenate(attended, axis=0)
    update = jnp.dot(attended, out_ref[...], preferred_element_type=jnp.float32)
    return (cells.astype(jnp.float32) + update).astype(jnp.bfloat16)


STEP = 4


def key_kernel(rows, *refs):
    feat_devices = lax.axis_size("feat")
    parts = refs[:feat_devices]
    feat_qkv, feat_out, item_qkv, out_ref, held, joined, key_ref, value_ref = refs[feat_devices:]
    feats = joined.shape[0] // rows
    width = joined.shape[1]
    assemble(parts, held, joined, rows)

    def one(step, carry):
        base = pl.multiple_of(step * (STEP * feats), STEP * feats)
        mixed = feature_rows(joined, base, STEP, feats, feat_qkv, feat_out)
        both = jnp.dot(mixed, item_qkv[:, width:], preferred_element_type=jnp.float32)
        key_ref[pl.ds(base, STEP * feats), :] = both[:, :width]
        value_ref[pl.ds(base, STEP * feats), :] = both[:, width:]
        return carry

    lax.fori_loop(0, rows // STEP, one, 0)
    for feat in range(feats):
        here = pl.ds(feat, rows, stride=feats)
        out_ref[feat, :, :width] = key_ref[here, :].astype(jnp.bfloat16)
        out_ref[feat, :, width:] = value_ref[here, :].astype(jnp.bfloat16)


def key_rows(parts, feat_qkv, feat_out, item_qkv):
    feat_devices = len(parts)
    rows = feat_devices * KEEP
    feats_here = parts[0].shape[0] // rows
    feats = feat_devices * feats_here
    width = parts[0].shape[1]
    return pl.pallas_call(
        functools.partial(key_kernel, rows),
        out_shape=jax.ShapeDtypeStruct((feats, rows, 2 * width), jnp.bfloat16),
        in_specs=[pl.BlockSpec(memory_space=pltpu.VMEM)] * (feat_devices + 3),
        out_specs=pl.BlockSpec(memory_space=pltpu.VMEM),
        scratch_shapes=[
            pltpu.VMEM((feat_devices, rows * feats_here, width), jnp.bfloat16),
            pltpu.VMEM((rows * feats, width), jnp.bfloat16),
            pltpu.VMEM((rows * feats, width), jnp.float32),
            pltpu.VMEM((rows * feats, width), jnp.float32),
        ],
        name="keys",
    )(*parts, feat_qkv, feat_out, item_qkv)


def row_kernel(rows, *refs):
    feat_devices = lax.axis_size("feat")
    parts = refs[:feat_devices]
    (feat_qkv, feat_out, item_qkv, item_out, keys_ref, bias_ref, out_ref) = refs[
        feat_devices : feat_devices + 7
    ]
    held, joined, mixed_ref, query_ref, item_ref = refs[feat_devices + 7 :]
    feats = joined.shape[0] // rows
    width = joined.shape[1]
    key_count = keys_ref.shape[1]
    assemble(parts, held, joined, rows)

    def one(step, carry):
        base = pl.multiple_of(step * (STEP * feats), STEP * feats)
        mixed = feature_rows(joined, base, STEP, feats, feat_qkv, feat_out)
        mixed_ref[pl.ds(base, STEP * feats), :] = mixed
        query_ref[pl.ds(base, STEP * feats), :] = jnp.dot(
            mixed, item_qkv[:, :width], preferred_element_type=jnp.float32
        )
        return carry

    lax.fori_loop(0, rows // STEP, one, 0)
    bias = bias_ref[:1, :key_count]
    masks = head_masks(rows, width)

    def item(step, carry):
        for inner in range(8):
            feat = step * 8 + inner
            queries = query_ref[pl.ds(feat, rows, stride=feats), :].astype(jnp.bfloat16)
            both = keys_ref[feat]
            item_ref[pl.ds(feat, rows, stride=feats), :] = attend(
                queries, both[:, :width], both[:, width:], (masks, masks), bias
            )
        return carry

    lax.fori_loop(0, feats // 8, item, 0)

    def last(step, carry):
        base = pl.multiple_of(step * (STEP * feats), STEP * feats)
        attended = item_ref[pl.ds(base, STEP * feats), :].astype(jnp.bfloat16)
        update = jnp.dot(attended, item_out[...], preferred_element_type=jnp.float32)
        result = (mixed_ref[pl.ds(base, STEP * feats), :].astype(jnp.float32) + update).astype(
            jnp.bfloat16
        )
        for row in range(STEP):
            out_ref[step * STEP + row] = result[row * feats : (row + 1) * feats]
        return carry

    lax.fori_loop(0, rows // STEP, last, 0)


def own_rows(parts, rows, feat_qkv, feat_out, item_qkv, item_out, keys, bias):
    feat_devices = len(parts)
    feats_here = parts[0].shape[0] // rows
    feats = feat_devices * feats_here
    width = parts[0].shape[1]
    return pl.pallas_call(
        functools.partial(row_kernel, rows),
        out_shape=jax.ShapeDtypeStruct((rows, feats, width), jnp.bfloat16),
        in_specs=[pl.BlockSpec(memory_space=pltpu.VMEM)] * (feat_devices + 6),
        out_specs=pl.BlockSpec(memory_space=pltpu.VMEM),
        scratch_shapes=[
            pltpu.VMEM((feat_devices, rows * feats_here, width), jnp.bfloat16),
            pltpu.VMEM((rows * feats, width), jnp.bfloat16),
            pltpu.VMEM((rows * feats, width), jnp.bfloat16),
            pltpu.VMEM((rows * feats, width), jnp.float32),
            pltpu.VMEM((rows * feats, width), jnp.float32),
        ],
        name="rows",
    )(*parts, feat_qkv, feat_out, item_qkv, item_out, keys, bias)


def swap(tensor, step):
    devices = lax.axis_size("feat")
    return lax.ppermute(tensor, "feat", [(one, one ^ step) for one in range(devices)])


CHUNKS = 1


def one_block_per_table(
    cells, block_table, row_live, row_train, feat_qkv, feat_out, item_qkv, item_out
):
    feat_devices = lax.axis_size("feat")
    group_rows = cells.shape[0] // feat_devices
    chunks = [group_rows // CHUNKS] * CHUNKS
    bias, train_rows, sends = prepare(cells, row_live, row_train, chunks)
    train_parts = [train_rows] + [swap(train_rows, step) for step in range(1, feat_devices)]
    row_parts = [
        [sends[0][at]] + [swap(sends[step][at], step) for step in range(1, feat_devices)]
        for at in range(len(chunks))
    ]
    keys = key_rows(train_parts, feat_qkv, feat_out, item_qkv)
    results = [
        own_rows(parts, size, feat_qkv, feat_out, item_qkv, item_out, keys, bias)
        for parts, size in zip(row_parts, chunks)
    ]
    return results[0] if len(results) == 1 else jnp.concatenate(results, axis=0)


def layer(cells, block_table, *rest):
    if block_table.shape[0] == TABLES:
        return one_block_per_table(cells, block_table, *rest)
    return on_device(cells, block_table, *rest)


def solution(mesh):
    return jax.shard_map(
        layer,
        mesh=mesh,
        in_specs=(P("rows", "feat", None), P(), P(), P(), P(), P(), P(), P()),
        out_specs=P(("rows", "feat"), None, None),
        check_vma=False,
    )
```

```python
import functools
import math

import jax
import jax.numpy as jnp
from jax import lax
from jax.experimental import pallas as pl
from jax.experimental.pallas import tpu as pltpu
from jax.sharding import PartitionSpec as P

HEADS = 4
HEAD_DIM = 32
KEEP = 4
TABLES = 8


EPSILON = 1e-05
MASKED = -1e30
SCALE2 = HEAD_DIM ** (-0.5) * math.log2(math.e)


def compact_train(train_rows):
    positions = jnp.arange(train_rows.shape[-1], dtype=jnp.int32)
    ordinal = jnp.cumsum(train_rows, axis=-1) - 1
    slot_ids = jnp.arange(KEEP, dtype=jnp.int32)
    matched = (train_rows[..., None, :] == 1) & (ordinal[..., None, :] == slot_ids[:, None])
    return jnp.sum(jnp.where(matched, positions, 0), axis=-1)


def into_heads(tensor):
    return tensor.reshape(tensor.shape[:-1] + (HEADS, HEAD_DIM))


def attend_features(queries, key_part, value_part):
    row_count, query_feats = (queries.shape[0], queries.shape[1])
    blocks = max(1, row_count * query_feats // 1280)
    while row_count % blocks:
        blocks -= 1
    scaling = HEAD_DIM ** (-0.5)

    def attend_one_block(block_parts):
        block_query, block_key, block_value = block_parts
        scores = (
            jnp.einsum(
                "rqhd,rkhd->rhqk", block_query, block_key, preferred_element_type=jnp.float32
            )
            * scaling
        )
        shares = jax.nn.softmax(scores, axis=-1).astype(jnp.bfloat16)
        return jnp.einsum(
            "rhqk,rkhd->rqhd", shares, block_value, preferred_element_type=jnp.float32
        ).astype(jnp.bfloat16)

    def by_block(tensor):
        return tensor.reshape((blocks, row_count // blocks) + tensor.shape[1:])

    result = lax.map(
        attend_one_block, (by_block(queries), by_block(key_part), by_block(value_part))
    )
    return result.reshape(row_count, query_feats, HEADS * HEAD_DIM)


def feature_layer(normed_cells, feat_out, key_part, value_part, queries):
    attended = attend_features(queries, key_part, value_part)
    update = jnp.dot(attended, feat_out, preferred_element_type=jnp.float32)
    return (normed_cells.astype(jnp.float32) + update).astype(jnp.bfloat16)


def on_device(cells, block_table, row_live, row_train, feat_qkv, feat_out, item_qkv, item_out):
    rows_here, feats_here, width_all = cells.shape
    row_index = lax.axis_index("rows")
    feat_index = lax.axis_index("feat")
    row_devices = lax.axis_size("rows")
    feat_devices = lax.axis_size("feat")
    my_table = lax.dynamic_index_in_dim(block_table, row_index, keepdims=False)
    live_rows = lax.dynamic_slice_in_dim(row_live, row_index * rows_here, rows_here).astype(
        jnp.float32
    )
    values = cells.astype(jnp.float32)
    table_hot = (jnp.arange(TABLES, dtype=jnp.int32) == my_table).astype(jnp.float32)
    first_local = jnp.sum(values * live_rows[:, None, None], axis=(0, 2))
    count_local = jnp.sum(live_rows) * width_all
    first_sum, count_sum = lax.psum(
        (table_hot[:, None] * first_local[None, :], table_hot * count_local), "rows"
    )
    table_mean = first_sum / count_sum[:, None]
    mine_mean = lax.dynamic_index_in_dim(table_mean, my_table, keepdims=False)
    centred = values - mine_mean[None, :, None]
    second_local = jnp.sum(centred * centred * live_rows[:, None, None], axis=(0, 2))
    second_sum = lax.psum(table_hot[:, None] * second_local[None, :], "rows")
    table_spread = second_sum / count_sum[:, None]
    mine_spread = lax.dynamic_index_in_dim(table_spread, my_table, keepdims=False)
    normed = (centred * lax.rsqrt(mine_spread + EPSILON)[None, :, None]).astype(jnp.bfloat16)
    normed_rows = lax.all_to_all(normed, "feat", split_axis=0, concat_axis=1, tiled=True)
    projected = jnp.dot(normed_rows, feat_qkv, preferred_element_type=jnp.float32).astype(
        jnp.bfloat16
    )
    queries = into_heads(projected[..., :width_all])
    key_part = into_heads(projected[..., width_all : 2 * width_all])
    value_part = into_heads(projected[..., 2 * width_all :])
    mixed_rows = feature_layer(normed_rows, feat_out, key_part, value_part, queries)
    group_rows, total_feats = (mixed_rows.shape[0], mixed_rows.shape[1])
    per_device = total_feats * HEADS // row_devices
    first_row = row_index * rows_here + feat_index * group_rows
    train_here = lax.dynamic_slice_in_dim(row_train, first_row, group_rows)
    places = compact_train(train_here)
    chosen = jnp.take(mixed_rows, places, axis=0)
    item_query = jnp.dot(
        mixed_rows, item_qkv[:, :width_all], preferred_element_type=jnp.float32
    ).astype(jnp.bfloat16)
    item_query = item_query.reshape(group_rows, row_devices, per_device, HEAD_DIM)
    key_value = jnp.dot(chosen, item_qkv[:, width_all:], preferred_element_type=jnp.float32).astype(
        jnp.bfloat16
    )
    item_key = key_value[..., :width_all].reshape(KEEP, row_devices, per_device, HEAD_DIM)
    item_value = key_value[..., width_all:].reshape(KEEP, row_devices, per_device, HEAD_DIM)
    query_table = jnp.repeat(block_table, group_rows)
    groups_all = row_train.reshape(row_devices, feat_devices, group_rows)
    group_counts = jnp.sum(groups_all, axis=2)
    slot_ids = jnp.arange(KEEP, dtype=jnp.int32)
    key_valid = slot_ids[None, None, :] < jnp.transpose(group_counts)[:, :, None]
    key_table = jnp.broadcast_to(block_table[None, :, None], key_valid.shape)
    allowed = (query_table[:, None] == key_table.reshape(-1)[None, :]) & key_valid.reshape(-1)[
        None, :
    ]
    query_count = query_table.shape[0]
    key_count = allowed.shape[1]
    query_blocks = max(1, query_count // 512)
    while query_count % query_blocks:
        query_blocks -= 1
    scaling = HEAD_DIM ** (-0.5)
    blocked_allowed = allowed.reshape(query_blocks, query_count // query_blocks, key_count)
    local_query = lax.all_to_all(item_query, "rows", split_axis=1, concat_axis=0, tiled=True)
    local_key = lax.all_to_all(item_key, "rows", split_axis=1, concat_axis=0, tiled=True)
    local_value = lax.all_to_all(item_value, "rows", split_axis=1, concat_axis=0, tiled=True)
    every_key = lax.all_gather(local_key, "feat", axis=0, tiled=True)
    every_value = lax.all_gather(local_value, "feat", axis=0, tiled=True)

    def one_item(item_parts):
        single_query, single_key, single_value = item_parts

        def one_one_block(block_parts):
            block_query, block_allowed = block_parts
            scores = (
                jnp.dot(block_query, single_key.T, preferred_element_type=jnp.float32) * scaling
            )
            scores = jnp.where(block_allowed, scores, MASKED)
            shares = jax.nn.softmax(scores, axis=-1).astype(jnp.bfloat16)
            return jnp.dot(shares, single_value, preferred_element_type=jnp.float32).astype(
                jnp.bfloat16
            )

        blocked_query = single_query.reshape(query_blocks, query_count // query_blocks, HEAD_DIM)
        return lax.map(one_one_block, (blocked_query, blocked_allowed)).reshape(
            query_count, HEAD_DIM
        )

    by_item = (
        jnp.moveaxis(local_query[:, 0], 1, 0),
        jnp.moveaxis(every_key[:, 0], 1, 0),
        jnp.moveaxis(every_value[:, 0], 1, 0),
    )
    result = jnp.moveaxis(lax.map(one_item, by_item), 0, 1)[:, None]
    attended = lax.all_to_all(result, "rows", split_axis=0, concat_axis=1, tiled=True)
    attended = attended.reshape(group_rows, total_feats, width_all)
    update = jnp.dot(attended, item_out, preferred_element_type=jnp.float32)
    return (mixed_rows.astype(jnp.float32) + update).astype(jnp.bfloat16)


def vmem_kernel(body, shapes, count, scratch, name, limit):
    many = isinstance(shapes, list)
    block = pl.BlockSpec(memory_space=pltpu.VMEM)
    return pl.pallas_call(
        body,
        out_shape=shapes,
        in_specs=[block] * count,
        out_specs=[block] * len(shapes) if many else block,
        scratch_shapes=scratch,
        compiler_params=pltpu.CompilerParams(vmem_limit_bytes=limit << 20),
        name=name,
    )


def prepare_kernel(chunks, live_ref, train_ref, cells_ref, bias_ref, train_out, *outs):
    feats_here, rows_here, width = cells_ref.shape
    feat_devices = lax.axis_size("feat")
    group_rows = rows_here // feat_devices
    feat_index = lax.axis_index("feat")
    row_index = lax.axis_index("rows")
    keys = train_out.shape[1]

    live = live_ref[pl.ds(row_index, 1), :].astype(jnp.float32)
    count = jnp.sum(live, axis=1, keepdims=True) * width
    weight = jnp.transpose(jnp.broadcast_to(live, (width, rows_here)))

    def total(values):
        return jnp.sum(jnp.sum(values, axis=0, keepdims=True), axis=1, keepdims=True)

    means = []
    for feat in range(feats_here):
        values = cells_ref[feat].astype(jnp.float32)
        means.append(jnp.broadcast_to(total(values * weight) / count, (1, width)))
    factors = []
    for feat in range(feats_here):
        centred = cells_ref[feat].astype(jnp.float32) - means[feat]
        spread = total(centred * centred * weight) / count
        factors.append(jnp.broadcast_to(lax.rsqrt(spread + EPSILON), (1, width)))

    train = jnp.broadcast_to(train_ref[pl.ds(row_index, 1), :], (keys, rows_here))
    before = lax.broadcasted_iota(jnp.int32, (rows_here, rows_here), 0)
    after = lax.broadcasted_iota(jnp.int32, (rows_here, rows_here), 1)
    ladder = (before <= after) & (before // group_rows == after // group_rows)
    ordinal = jnp.dot(
        train.astype(jnp.float32).astype(jnp.bfloat16),
        jnp.where(ladder, 1.0, 0.0).astype(jnp.bfloat16),
        preferred_element_type=jnp.float32,
    )
    key = lax.broadcasted_iota(jnp.int32, (keys, rows_here), 0)
    row = lax.broadcasted_iota(jnp.int32, (keys, rows_here), 1)
    here = (
        (train == 1)
        & (row // group_rows == key // KEEP)
        & (ordinal == (key % KEEP + 1).astype(jnp.float32))
    )
    chosen = jnp.where(here, 1.0, 0.0)
    found = jnp.sum(chosen, axis=1, keepdims=True)
    bias_ref[...] = jnp.broadcast_to(jnp.where(found > 0.5, 0.0, MASKED), bias_ref.shape)
    chosen = chosen.astype(jnp.bfloat16)

    def normed(feat, values):
        centred = values.astype(jnp.float32) - means[feat]
        return (centred * factors[feat]).astype(jnp.bfloat16)

    for feat in range(feats_here):
        train_out[feat] = jnp.dot(
            chosen, normed(feat, cells_ref[feat]), preferred_element_type=jnp.float32
        ).astype(jnp.bfloat16)
    for step in range(feat_devices):
        done = 0
        for at, size in enumerate(chunks):
            first_row = pl.multiple_of((feat_index ^ step) * group_rows + done, 16)
            for feat in range(feats_here):
                outs[step * len(chunks) + at][feat] = normed(
                    feat, cells_ref[feat, pl.ds(first_row, size), :]
                )
            done += size


def prepare(cells, row_live, row_train, chunks):
    rows_here, feats_here, width = cells.shape
    feat_devices = lax.axis_size("feat")
    keys = feat_devices * KEEP
    shapes = [
        jax.ShapeDtypeStruct((keys, 128), jnp.float32),
        jax.ShapeDtypeStruct((feats_here, keys, width), jnp.bfloat16),
    ]
    for _ in range(feat_devices):
        for size in chunks:
            shapes.append(jax.ShapeDtypeStruct((feats_here, size, width), jnp.bfloat16))
    outs = vmem_kernel(
        functools.partial(prepare_kernel, chunks), shapes, 3, [], "prepare", 8
    )(
        row_live.reshape(-1, rows_here),
        row_train.reshape(-1, rows_here),
        jnp.transpose(cells, (1, 0, 2)),
    )
    sends = [
        [outs[2 + step * len(chunks) + at] for at in range(len(chunks))]
        for step in range(feat_devices)
    ]
    return outs[0], outs[1], sends


def gather_parts(parts, held):
    feat_index = lax.axis_index("feat")
    feats_here, rows, width = parts[0].shape
    size = feats_here * rows
    for step, part in enumerate(parts):
        start = pl.multiple_of((feat_index ^ step) * size, size)
        held[pl.ds(start, size), :] = part[...].reshape(size, width).astype(jnp.float32)


def head_masks(rows, width):
    lane = lax.broadcasted_iota(jnp.int32, (rows, width), 1)
    return [(lane // HEAD_DIM) == head for head in range(HEADS)]


def by_head(tensor, masks):
    return [jnp.where(mask, tensor, jnp.zeros_like(tensor)) for mask in masks]


def attend(queries, keys, values, masks):
    count, width = queries.shape
    scores = lax.dot_general(
        jnp.concatenate(by_head(queries, masks), axis=0),
        keys,
        (((1,), (1,)), ((), ())),
        preferred_element_type=jnp.float32,
    )
    top = jnp.max(scores, axis=1, keepdims=True)
    shares = jnp.exp2((scores - top) * SCALE2).astype(jnp.bfloat16)
    both = jnp.concatenate([values, jnp.ones_like(values)], axis=1)
    mixed = jnp.dot(shares, both, preferred_element_type=jnp.float32)
    out, total = mixed[:count, :width], mixed[:count, width:]
    for head in range(1, HEADS):
        block = mixed[head * count : (head + 1) * count]
        out = jnp.where(masks[head], block[:, :width], out)
        total = jnp.where(masks[head], block[:, width:], total)
    return out / total


def feature_rows(held, first, rows, stride, qkv_ref, out_ref):
    feats = held.shape[0] // stride
    width = held.shape[1]
    cells = jnp.concatenate(
        [held[pl.ds(first + row, feats, stride=stride), :] for row in range(rows)], axis=0
    )
    projected = jnp.dot(
        cells.astype(jnp.bfloat16), qkv_ref[...], preferred_element_type=jnp.float32
    ).astype(jnp.bfloat16)
    masks = head_masks(feats, width)
    attended = []
    for row in range(rows):
        block = projected[row * feats : (row + 1) * feats]
        attended.append(
            attend(
                block[:, :width],
                block[:, width : 2 * width],
                block[:, 2 * width :],
                masks,
            ).astype(jnp.bfloat16)
        )
    attended = jnp.concatenate(attended, axis=0)
    update = jnp.dot(attended, out_ref[...], preferred_element_type=jnp.float32)
    return (cells + update).astype(jnp.bfloat16)


STEP = 16


def key_kernel(*refs):
    feat_devices = lax.axis_size("feat")
    parts = refs[:feat_devices]
    feat_qkv, feat_out, item_qkv, out_ref, held, key_ref, value_ref = refs[feat_devices:]
    rows = parts[0].shape[1]
    feats, width = held.shape[0] // rows, held.shape[1]
    step_rows = math.gcd(rows, STEP)
    gather_parts(parts, held)

    def one(step, carry):
        mixed = feature_rows(held, step * step_rows, step_rows, rows, feat_qkv, feat_out)
        both = jnp.dot(mixed, item_qkv[:, width:], preferred_element_type=jnp.float32)
        here = pl.ds(pl.multiple_of(step * (step_rows * feats), step_rows * feats), step_rows * feats)
        key_ref[here, :] = both[:, :width]
        value_ref[here, :] = both[:, width:]
        return carry

    lax.fori_loop(0, rows // step_rows, one, 0)
    for feat in range(feats):
        here = pl.ds(feat, rows, stride=feats)
        out_ref[feat, :, :width] = key_ref[here, :].astype(jnp.bfloat16)
        out_ref[feat, :, width:] = value_ref[here, :].astype(jnp.bfloat16)


def key_rows(parts, feat_qkv, feat_out, item_qkv):
    feats_here, rows, width = parts[0].shape
    feats = len(parts) * feats_here
    table = pltpu.VMEM((rows * feats, width), jnp.float32)
    return vmem_kernel(
        key_kernel,
        jax.ShapeDtypeStruct((feats, rows, 2 * width), jnp.bfloat16),
        len(parts) + 3,
        [table, table, table],
        "keys",
        24,
    )(*parts, feat_qkv, feat_out, item_qkv)


def row_kernel(*refs):
    feat_devices = lax.axis_size("feat")
    parts = refs[:feat_devices]
    (feat_qkv, feat_out, item_qkv, item_out, keys_ref, bias_ref, out_ref) = refs[
        feat_devices : feat_devices + 7
    ]
    held, mixed_ref, query_ref, item_ref = refs[feat_devices + 7 :]
    rows = parts[0].shape[1]
    feats, width = held.shape[0] // rows, held.shape[1]
    step_rows = math.gcd(rows, STEP)
    keys = keys_ref.shape[1]
    gather_parts(parts, held)

    def span(step):
        return pl.ds(pl.multiple_of(step * (step_rows * feats), step_rows * feats), step_rows * feats)

    def one(step, carry):
        mixed = feature_rows(held, step * step_rows, step_rows, rows, feat_qkv, feat_out)
        mixed_ref[span(step), :] = mixed
        query_ref[span(step), :] = jnp.dot(
            mixed, item_qkv[:, :width], preferred_element_type=jnp.float32
        )
        return carry

    lax.fori_loop(0, rows // step_rows, one, 0)

    together = 128 // rows
    lanes = together * rows
    pairs = together // 2
    key_masks = head_masks(keys, width)
    bias = jnp.concatenate([bias_ref[:, :lanes]] * HEADS, axis=0)
    lane_owner = lax.broadcasted_iota(jnp.int32, (HEADS * keys, lanes), 1) // rows
    pair_row = lax.broadcasted_iota(jnp.int32, (2 * rows, 2 * HEADS * keys), 0) // rows
    pair_lane = lax.broadcasted_iota(jnp.int32, (2 * rows, 2 * HEADS * keys), 1) // (HEADS * keys)
    pair_mask = pair_row == pair_lane

    def item(step):
        queries, stacked_keys, stacked_values = [], [], []
        for inner in range(together):
            feat = step * together + inner
            queries.append(query_ref[pl.ds(feat, rows, stride=feats), :].astype(jnp.bfloat16))
            stacked_keys += by_head(keys_ref[feat, :, :width], key_masks)
            stacked_values += by_head(keys_ref[feat, :, width:], key_masks)
        every = lax.dot_general(
            jnp.concatenate(stacked_keys, axis=0),
            jnp.concatenate(queries, axis=0),
            (((1,), (1,)), ((), ())),
            preferred_element_type=jnp.float32,
        )
        size = HEADS * keys
        scores = every[:size]
        for inner in range(1, together):
            scores = jnp.where(lane_owner == inner, every[inner * size : (inner + 1) * size], scores)
        scores = (scores + bias).reshape(HEADS, keys, lanes)
        top = jnp.max(scores, axis=1, keepdims=True)
        powers = jnp.exp2((scores - top) * SCALE2)
        shares = powers / jnp.sum(powers, axis=1, keepdims=True)
        shares = shares.reshape(size, lanes)
        shares = jnp.transpose(jnp.concatenate([shares, shares], axis=0)).astype(jnp.bfloat16)
        for pair in range(pairs):
            block = shares[pair * 2 * rows : (pair + 1) * 2 * rows]
            result = jnp.dot(
                jnp.where(pair_mask, block, jnp.zeros_like(block)),
                jnp.concatenate(
                    stacked_values[pair * 2 * HEADS : (pair + 1) * 2 * HEADS], axis=0
                ),
                preferred_element_type=jnp.float32,
            )
            for inner in range(2):
                feat = step * together + pair * 2 + inner
                item_ref[pl.ds(feat, rows, stride=feats), :] = result[
                    inner * rows : (inner + 1) * rows
                ]

    def items(step, carry):
        for inner in range(ITEM_STEP):
            item(step * ITEM_STEP + inner)
        return carry

    lax.fori_loop(0, feats // (together * ITEM_STEP), items, 0)

    def last(step, carry):
        attended = item_ref[span(step), :].astype(jnp.bfloat16)
        update = jnp.dot(attended, item_out[...], preferred_element_type=jnp.float32)
        result = (mixed_ref[span(step), :].astype(jnp.float32) + update).astype(jnp.bfloat16)
        for row in range(step_rows):
            out_ref[step * step_rows + row] = result[row * feats : (row + 1) * feats]
        return carry

    lax.fori_loop(0, rows // step_rows, last, 0)


ITEM_STEP = 4


def own_rows(parts, feat_qkv, feat_out, item_qkv, item_out, keys, bias):
    feats_here, rows, width = parts[0].shape
    feats = len(parts) * feats_here
    table = pltpu.VMEM((rows * feats, width), jnp.float32)
    return vmem_kernel(
        row_kernel,
        jax.ShapeDtypeStruct((rows, feats, width), jnp.bfloat16),
        len(parts) + 6,
        [table, pltpu.VMEM((rows * feats, width), jnp.bfloat16), table, table],
        "rows",
        24,
    )(*parts, feat_qkv, feat_out, item_qkv, item_out, keys, bias)


def swap(tensor, step):
    devices = lax.axis_size("feat")
    return lax.ppermute(tensor, "feat", [(one, one ^ step) for one in range(devices)])


CHUNKS = 1


def one_block_per_table(
    cells, block_table, row_live, row_train, feat_qkv, feat_out, item_qkv, item_out
):
    feat_devices = lax.axis_size("feat")
    group_rows = cells.shape[0] // feat_devices
    chunks = [group_rows // CHUNKS] * CHUNKS
    bias, train_rows, sends = prepare(cells, row_live, row_train, chunks)
    train_parts = [train_rows] + [swap(train_rows, step) for step in range(1, feat_devices)]
    row_parts = [
        [sends[0][at]] + [swap(sends[step][at], step) for step in range(1, feat_devices)]
        for at in range(len(chunks))
    ]
    keys = key_rows(train_parts, feat_qkv, feat_out, item_qkv)
    results = [
        own_rows(parts, feat_qkv, feat_out, item_qkv, item_out, keys, bias)
        for parts in row_parts
    ]
    return results[0] if len(results) == 1 else jnp.concatenate(results, axis=0)


def layer(cells, block_table, *rest):
    if block_table.shape[0] == TABLES:
        return one_block_per_table(cells, block_table, *rest)
    return on_device(cells, block_table, *rest)


def solution(mesh):
    return jax.shard_map(
        layer,
        mesh=mesh,
        in_specs=(P("rows", "feat", None), P(), P(), P(), P(), P(), P(), P()),
        out_specs=P(("rows", "feat"), None, None),
        check_vma=False,
    )
```

```python
import functools
import math

import jax
import jax.numpy as jnp
from jax import lax
from jax.experimental import pallas as pl
from jax.experimental.pallas import tpu as pltpu
from jax.sharding import PartitionSpec as P

HEADS = 4
HEAD_DIM = 32
KEEP = 4
TABLES = 8


EPSILON = 1e-05
MASKED = -1e30
SCALE2 = HEAD_DIM ** (-0.5) * math.log2(math.e)


def compact_train(train_rows):
    positions = jnp.arange(train_rows.shape[-1], dtype=jnp.int32)
    ordinal = jnp.cumsum(train_rows, axis=-1) - 1
    slot_ids = jnp.arange(KEEP, dtype=jnp.int32)
    matched = (train_rows[..., None, :] == 1) & (ordinal[..., None, :] == slot_ids[:, None])
    return jnp.sum(jnp.where(matched, positions, 0), axis=-1)


def into_heads(tensor):
    return tensor.reshape(tensor.shape[:-1] + (HEADS, HEAD_DIM))


def attend_features(queries, key_part, value_part):
    row_count, query_feats = (queries.shape[0], queries.shape[1])
    blocks = max(1, row_count * query_feats // 1280)
    while row_count % blocks:
        blocks -= 1
    scaling = HEAD_DIM ** (-0.5)

    def attend_one_block(block_parts):
        block_query, block_key, block_value = block_parts
        scores = (
            jnp.einsum(
                "rqhd,rkhd->rhqk", block_query, block_key, preferred_element_type=jnp.float32
            )
            * scaling
        )
        shares = jax.nn.softmax(scores, axis=-1).astype(jnp.bfloat16)
        return jnp.einsum(
            "rhqk,rkhd->rqhd", shares, block_value, preferred_element_type=jnp.float32
        ).astype(jnp.bfloat16)

    def by_block(tensor):
        return tensor.reshape((blocks, row_count // blocks) + tensor.shape[1:])

    result = lax.map(
        attend_one_block, (by_block(queries), by_block(key_part), by_block(value_part))
    )
    return result.reshape(row_count, query_feats, HEADS * HEAD_DIM)


def feature_layer(normed_cells, feat_out, key_part, value_part, queries):
    attended = attend_features(queries, key_part, value_part)
    update = jnp.dot(attended, feat_out, preferred_element_type=jnp.float32)
    return (normed_cells.astype(jnp.float32) + update).astype(jnp.bfloat16)


def on_device(cells, block_table, row_live, row_train, feat_qkv, feat_out, item_qkv, item_out):
    rows_here, _, width_all = cells.shape
    row_index = lax.axis_index("rows")
    feat_index = lax.axis_index("feat")
    row_devices = lax.axis_size("rows")
    feat_devices = lax.axis_size("feat")
    my_table = lax.dynamic_index_in_dim(block_table, row_index, keepdims=False)
    live_rows = lax.dynamic_slice_in_dim(row_live, row_index * rows_here, rows_here).astype(
        jnp.float32
    )
    values = cells.astype(jnp.float32)
    table_hot = (jnp.arange(TABLES, dtype=jnp.int32) == my_table).astype(jnp.float32)
    first_local = jnp.sum(values * live_rows[:, None, None], axis=(0, 2))
    count_local = jnp.sum(live_rows) * width_all
    first_sum, count_sum = lax.psum(
        (table_hot[:, None] * first_local[None, :], table_hot * count_local), "rows"
    )
    table_mean = first_sum / count_sum[:, None]
    mine_mean = lax.dynamic_index_in_dim(table_mean, my_table, keepdims=False)
    centred = values - mine_mean[None, :, None]
    second_local = jnp.sum(centred * centred * live_rows[:, None, None], axis=(0, 2))
    second_sum = lax.psum(table_hot[:, None] * second_local[None, :], "rows")
    table_spread = second_sum / count_sum[:, None]
    mine_spread = lax.dynamic_index_in_dim(table_spread, my_table, keepdims=False)
    normed = (centred * lax.rsqrt(mine_spread + EPSILON)[None, :, None]).astype(jnp.bfloat16)
    normed_rows = lax.all_to_all(normed, "feat", split_axis=0, concat_axis=1, tiled=True)
    projected = jnp.dot(normed_rows, feat_qkv, preferred_element_type=jnp.float32).astype(
        jnp.bfloat16
    )
    queries = into_heads(projected[..., :width_all])
    key_part = into_heads(projected[..., width_all : 2 * width_all])
    value_part = into_heads(projected[..., 2 * width_all :])
    mixed_rows = feature_layer(normed_rows, feat_out, key_part, value_part, queries)
    group_rows, total_feats = (mixed_rows.shape[0], mixed_rows.shape[1])
    per_device = total_feats * HEADS // row_devices
    first_row = row_index * rows_here + feat_index * group_rows
    train_here = lax.dynamic_slice_in_dim(row_train, first_row, group_rows)
    places = compact_train(train_here)
    chosen = jnp.take(mixed_rows, places, axis=0)
    item_query = jnp.dot(
        mixed_rows, item_qkv[:, :width_all], preferred_element_type=jnp.float32
    ).astype(jnp.bfloat16)
    item_query = item_query.reshape(group_rows, row_devices, per_device, HEAD_DIM)
    key_value = jnp.dot(chosen, item_qkv[:, width_all:], preferred_element_type=jnp.float32).astype(
        jnp.bfloat16
    )
    item_key = key_value[..., :width_all].reshape(KEEP, row_devices, per_device, HEAD_DIM)
    item_value = key_value[..., width_all:].reshape(KEEP, row_devices, per_device, HEAD_DIM)
    query_table = jnp.repeat(block_table, group_rows)
    groups_all = row_train.reshape(row_devices, feat_devices, group_rows)
    group_counts = jnp.sum(groups_all, axis=2)
    slot_ids = jnp.arange(KEEP, dtype=jnp.int32)
    key_valid = slot_ids[None, None, :] < jnp.transpose(group_counts)[:, :, None]
    key_table = jnp.broadcast_to(block_table[None, :, None], key_valid.shape)
    allowed = (query_table[:, None] == key_table.reshape(-1)[None, :]) & key_valid.reshape(-1)[
        None, :
    ]
    query_count = query_table.shape[0]
    key_count = allowed.shape[1]
    query_blocks = max(1, query_count // 512)
    while query_count % query_blocks:
        query_blocks -= 1
    scaling = HEAD_DIM ** (-0.5)
    blocked_allowed = allowed.reshape(query_blocks, query_count // query_blocks, key_count)
    local_query = lax.all_to_all(item_query, "rows", split_axis=1, concat_axis=0, tiled=True)
    local_key = lax.all_to_all(item_key, "rows", split_axis=1, concat_axis=0, tiled=True)
    local_value = lax.all_to_all(item_value, "rows", split_axis=1, concat_axis=0, tiled=True)
    every_key = lax.all_gather(local_key, "feat", axis=0, tiled=True)
    every_value = lax.all_gather(local_value, "feat", axis=0, tiled=True)

    def one_item(item_parts):
        single_query, single_key, single_value = item_parts

        def one_one_block(block_parts):
            block_query, block_allowed = block_parts
            scores = (
                jnp.dot(block_query, single_key.T, preferred_element_type=jnp.float32) * scaling
            )
            scores = jnp.where(block_allowed, scores, MASKED)
            shares = jax.nn.softmax(scores, axis=-1).astype(jnp.bfloat16)
            return jnp.dot(shares, single_value, preferred_element_type=jnp.float32).astype(
                jnp.bfloat16
            )

        blocked_query = single_query.reshape(query_blocks, query_count // query_blocks, HEAD_DIM)
        return lax.map(one_one_block, (blocked_query, blocked_allowed)).reshape(
            query_count, HEAD_DIM
        )

    by_item = (
        jnp.moveaxis(local_query[:, 0], 1, 0),
        jnp.moveaxis(every_key[:, 0], 1, 0),
        jnp.moveaxis(every_value[:, 0], 1, 0),
    )
    result = jnp.moveaxis(lax.map(one_item, by_item), 0, 1)[:, None]
    attended = lax.all_to_all(result, "rows", split_axis=0, concat_axis=1, tiled=True)
    attended = attended.reshape(group_rows, total_feats, width_all)
    update = jnp.dot(attended, item_out, preferred_element_type=jnp.float32)
    return (mixed_rows.astype(jnp.float32) + update).astype(jnp.bfloat16)


def vmem_kernel(body, shapes, count, scratch, limit):
    many = isinstance(shapes, list)
    block = pl.BlockSpec(memory_space=pltpu.VMEM)
    return pl.pallas_call(
        body,
        out_shape=shapes,
        in_specs=[block] * count,
        out_specs=[block] * len(shapes) if many else block,
        scratch_shapes=scratch,
        compiler_params=pltpu.CompilerParams(vmem_limit_bytes=limit << 20),
    )


PIECES = 4


def prepare_kernel(chunks, live_in, train_in, cells_in, bias_ref, train_out, *refs):
    outs, (live_ref, train_ref, cells_ref, sems) = refs[:-4], refs[-4:]
    feats_here, rows_here, width = cells_ref.shape
    feat_devices = lax.axis_size("feat")
    group_rows = rows_here // feat_devices
    feat_index = lax.axis_index("feat")
    row_index = lax.axis_index("rows")
    keys = train_out.shape[1]
    piece = feats_here // math.gcd(feats_here, PIECES)

    copies = [
        pltpu.make_async_copy(live_in, live_ref, sems.at[0]),
        pltpu.make_async_copy(train_in, train_ref, sems.at[1]),
    ]
    for at, feat in enumerate(range(0, feats_here, piece)):
        here = pl.ds(feat, piece)
        copies.append(
            pltpu.make_async_copy(cells_in.at[here], cells_ref.at[here], sems.at[2 + at])
        )
    for copy in copies:
        copy.start()
    for copy in copies[:2]:
        copy.wait()

    live = live_ref[pl.ds(row_index, 1), :].astype(jnp.float32)
    count = jnp.sum(live, axis=1, keepdims=True) * width
    weight = jnp.transpose(jnp.broadcast_to(live, (width, rows_here)))

    def total(values):
        return jnp.sum(jnp.sum(values, axis=0, keepdims=True), axis=1, keepdims=True)

    means = []
    for feat in range(feats_here):
        if feat % piece == 0:
            copies[2 + feat // piece].wait()
        values = cells_ref[feat].astype(jnp.float32)
        means.append(jnp.broadcast_to(total(values * weight) / count, (1, width)))
    factors = []
    for feat in range(feats_here):
        centred = cells_ref[feat].astype(jnp.float32) - means[feat]
        spread = total(centred * centred * weight) / count
        factors.append(jnp.broadcast_to(lax.rsqrt(spread + EPSILON), (1, width)))

    train = jnp.broadcast_to(train_ref[pl.ds(row_index, 1), :], (keys, rows_here))
    before = lax.broadcasted_iota(jnp.int32, (rows_here, rows_here), 0)
    after = lax.broadcasted_iota(jnp.int32, (rows_here, rows_here), 1)
    ladder = (before <= after) & (before // group_rows == after // group_rows)
    ordinal = jnp.dot(
        train.astype(jnp.float32).astype(jnp.bfloat16),
        jnp.where(ladder, 1.0, 0.0).astype(jnp.bfloat16),
        preferred_element_type=jnp.float32,
    )
    key = lax.broadcasted_iota(jnp.int32, (keys, rows_here), 0)
    row = lax.broadcasted_iota(jnp.int32, (keys, rows_here), 1)
    here = (
        (train == 1)
        & (row // group_rows == key // KEEP)
        & (ordinal == (key % KEEP + 1).astype(jnp.float32))
    )
    chosen = jnp.where(here, 1.0, 0.0)
    found = jnp.sum(chosen, axis=1, keepdims=True)
    bias_ref[...] = jnp.broadcast_to(jnp.where(found > 0.5, 0.0, MASKED), bias_ref.shape)
    chosen = chosen.astype(jnp.bfloat16)

    def normed(feat, values):
        centred = values.astype(jnp.float32) - means[feat]
        return (centred * factors[feat]).astype(jnp.bfloat16)

    near_out = outs[0]
    for feat in range(feats_here):
        rows = jnp.dot(
            chosen, normed(feat, cells_ref[feat]), preferred_element_type=jnp.float32
        ).astype(jnp.bfloat16)
        train_out[feat] = rows
        near_out[0, feat] = rows
    for step in range(feat_devices):
        for at in range(chunks):
            size = group_rows // chunks
            first_row = pl.multiple_of((feat_index ^ step) * group_rows + at * size, size)
            for feat in range(feats_here):
                rows = normed(feat, cells_ref[feat, pl.ds(first_row, size), :])
                if step == 1:
                    near_out[1 + at, feat] = rows
                else:
                    outs[1 + max(step - 1, 0) * chunks + at][feat] = rows


def prepare(cells, row_live, row_train, chunks):
    rows_here, feats_here, width = cells.shape
    feat_devices = lax.axis_size("feat")
    keys = feat_devices * KEEP
    shapes = [
        jax.ShapeDtypeStruct((keys, 128), jnp.float32),
        jax.ShapeDtypeStruct((feats_here, keys, width), jnp.bfloat16),
    ]
    size = rows_here // feat_devices // chunks
    assert size == keys
    part = jax.ShapeDtypeStruct((feats_here, size, width), jnp.bfloat16)
    shapes.append(jax.ShapeDtypeStruct((1 + chunks,) + part.shape, jnp.bfloat16))
    shapes += [part] * ((feat_devices - 1) * chunks)
    blocks = row_live.shape[0] // rows_here
    block = pl.BlockSpec(memory_space=pltpu.VMEM)
    outs = pl.pallas_call(
        functools.partial(prepare_kernel, chunks),
        out_shape=shapes,
        in_specs=[pl.BlockSpec(memory_space=pltpu.HBM)] * 3,
        out_specs=[block] * len(shapes),
        scratch_shapes=[
            pltpu.VMEM((blocks, rows_here), jnp.int32),
            pltpu.VMEM((blocks, rows_here), jnp.int32),
            pltpu.VMEM((feats_here, rows_here, width), jnp.bfloat16),
            pltpu.SemaphoreType.DMA((2 + math.gcd(feats_here, PIECES),)),
        ],
        compiler_params=pltpu.CompilerParams(vmem_limit_bytes=8 << 20),
        name="prepare",
    )(
        pltpu.with_memory_space_constraint(row_live.reshape(-1, rows_here), pltpu.HBM),
        pltpu.with_memory_space_constraint(row_train.reshape(-1, rows_here), pltpu.HBM),
        pltpu.with_memory_space_constraint(jnp.transpose(cells, (1, 0, 2)), pltpu.HBM),
    )
    sends = {
        step: outs[3 + at * chunks : 3 + (at + 1) * chunks]
        for at, step in enumerate([0, *range(2, feat_devices)])
    }
    return outs[0], outs[1], outs[2], sends


def gather_parts(parts, at, held):
    feat_index = lax.axis_index("feat")
    feats_here, rows, width = parts[0].shape
    size = feats_here * rows
    for step, part in enumerate(parts):
        start = pl.multiple_of((feat_index ^ step) * size, size)
        values = part[at] if step == 1 else part[...]
        held[pl.ds(start, size), :] = values.reshape(size, width).astype(jnp.float32)


def head_masks(rows, width):
    lane = lax.broadcasted_iota(jnp.int32, (rows, width), 1)
    return [(lane // HEAD_DIM) == head for head in range(HEADS)]


def by_head(tensor, masks):
    return [jnp.where(mask, tensor, jnp.zeros_like(tensor)) for mask in masks]


def attend(queries, keys, values, masks):
    count, width = queries.shape
    half = width // 2
    scores = lax.dot_general(
        jnp.concatenate(by_head(queries, masks), axis=0),
        keys,
        (((1,), (1,)), ((), ())),
        preferred_element_type=jnp.float32,
    )
    top = jnp.max(scores, axis=1, keepdims=True)
    shares = jnp.exp2((scores - top) * SCALE2).astype(jnp.bfloat16)
    lane = lax.broadcasted_iota(jnp.int32, (count, width), 1)
    low, ones = lane < half, jnp.ones_like(values)
    sides = []
    for side in range(2):
        first = side * (HEADS // 2)
        both = jnp.where(low, values, ones) if side == 0 else jnp.where(low, ones, values)
        mixed = jnp.dot(
            shares[first * count : (first + HEADS // 2) * count],
            both,
            preferred_element_type=jnp.float32,
        )
        picked = mixed[:count]
        for head in range(1, HEADS // 2):
            mine = (lane % half) // HEAD_DIM == head
            picked = jnp.where(mine, mixed[head * count : (head + 1) * count], picked)
        sides.append(picked)
    out = jnp.where(low, sides[0], sides[1])
    total = pltpu.roll(jnp.where(low, sides[1], sides[0]), half, 1)
    return out / total


def feature_rows(held, first, rows, stride, qkv_ref, out_ref):
    feats = held.shape[0] // stride
    width = held.shape[1]
    cells = jnp.concatenate(
        [held[pl.ds(first + row, feats, stride=stride), :] for row in range(rows)], axis=0
    )
    projected = jnp.dot(
        cells.astype(jnp.bfloat16), qkv_ref[...], preferred_element_type=jnp.float32
    ).astype(jnp.bfloat16)
    masks = head_masks(feats, width)
    attended = []
    for row in range(rows):
        block = projected[row * feats : (row + 1) * feats]
        attended.append(
            attend(
                block[:, :width],
                block[:, width : 2 * width],
                block[:, 2 * width :],
                masks,
            ).astype(jnp.bfloat16)
        )
    attended = jnp.concatenate(attended, axis=0)
    update = jnp.dot(attended, out_ref[...], preferred_element_type=jnp.float32)
    return (cells + update).astype(jnp.bfloat16)


STEP = 16


def key_kernel(*refs):
    feat_devices = lax.axis_size("feat")
    parts = refs[:feat_devices]
    feat_qkv, feat_out, item_qkv, out_ref, held, key_ref, value_ref = refs[feat_devices:]
    rows = parts[0].shape[1]
    feats, width = held.shape[0] // rows, held.shape[1]
    step_rows = math.gcd(rows, STEP)
    gather_parts(parts, 0, held)

    def one(step, carry):
        mixed = feature_rows(held, step * step_rows, step_rows, rows, feat_qkv, feat_out)
        both = jnp.dot(mixed, item_qkv[:, width:], preferred_element_type=jnp.float32)
        here = pl.ds(pl.multiple_of(step * (step_rows * feats), step_rows * feats), step_rows * feats)
        key_ref[here, :] = both[:, :width]
        value_ref[here, :] = both[:, width:]
        return carry

    lax.fori_loop(0, rows // step_rows, one, 0)
    for feat in range(feats):
        here = pl.ds(feat, rows, stride=feats)
        out_ref[feat, :, :width] = key_ref[here, :].astype(jnp.bfloat16)
        out_ref[feat, :, width:] = value_ref[here, :].astype(jnp.bfloat16)


def key_rows(parts, feat_qkv, feat_out, item_qkv):
    feats_here, rows, width = parts[0].shape
    feats = len(parts) * feats_here
    table = pltpu.VMEM((rows * feats, width), jnp.float32)
    return vmem_kernel(
        key_kernel,
        jax.ShapeDtypeStruct((feats, rows, 2 * width), jnp.bfloat16),
        len(parts) + 3,
        [table, table, table],
        24,
    )(*parts, feat_qkv, feat_out, item_qkv)


def row_kernel(first_row, aliased, *refs):
    feat_devices = lax.axis_size("feat")
    parts = refs[:feat_devices]
    (feat_qkv, feat_out, item_qkv, item_out, keys_ref, bias_ref) = refs[
        feat_devices : feat_devices + 6
    ]
    out_ref, held, mixed_ref, query_ref, item_ref, result_ref, sem = refs[
        feat_devices + 6 + aliased :
    ]
    rows = parts[0].shape[1]
    feats, width = held.shape[0] // rows, held.shape[1]
    step_rows = math.gcd(rows, STEP)
    keys = keys_ref.shape[1]
    gather_parts(parts, 1 + first_row // parts[0].shape[1], held)

    def span(step):
        return pl.ds(pl.multiple_of(step * (step_rows * feats), step_rows * feats), step_rows * feats)

    def one(step, carry):
        mixed = feature_rows(held, step * step_rows, step_rows, rows, feat_qkv, feat_out)
        mixed_ref[span(step), :] = mixed
        query_ref[span(step), :] = jnp.dot(
            mixed, item_qkv[:, :width], preferred_element_type=jnp.float32
        )
        return carry

    lax.fori_loop(0, rows // step_rows, one, 0)

    together = 128 // rows
    lanes = together * rows
    pairs = together // 2
    key_masks = head_masks(keys, width)
    bias = jnp.concatenate([bias_ref[:, :lanes]] * HEADS, axis=0)
    lane_owner = lax.broadcasted_iota(jnp.int32, (HEADS * keys, lanes), 1) // rows
    pair_row = lax.broadcasted_iota(jnp.int32, (2 * rows, 2 * HEADS * keys), 0) // rows
    pair_lane = lax.broadcasted_iota(jnp.int32, (2 * rows, 2 * HEADS * keys), 1) // (HEADS * keys)
    pair_mask = pair_row == pair_lane

    def item(step):
        queries, stacked_keys, stacked_values = [], [], []
        for inner in range(together):
            feat = step * together + inner
            queries.append(query_ref[pl.ds(feat, rows, stride=feats), :].astype(jnp.bfloat16))
            stacked_keys += by_head(keys_ref[feat, :, :width], key_masks)
            stacked_values += by_head(keys_ref[feat, :, width:], key_masks)
        every = lax.dot_general(
            jnp.concatenate(stacked_keys, axis=0),
            jnp.concatenate(queries, axis=0),
            (((1,), (1,)), ((), ())),
            preferred_element_type=jnp.float32,
        )
        size = HEADS * keys
        scores = every[:size]
        for inner in range(1, together):
            scores = jnp.where(lane_owner == inner, every[inner * size : (inner + 1) * size], scores)
        scores = (scores + bias).reshape(HEADS, keys, lanes)
        top = jnp.max(scores, axis=1, keepdims=True)
        powers = jnp.exp2((scores - top) * SCALE2)
        shares = powers / jnp.sum(powers, axis=1, keepdims=True)
        shares = shares.reshape(size, lanes)
        shares = jnp.transpose(jnp.concatenate([shares, shares], axis=0)).astype(jnp.bfloat16)
        for pair in range(pairs):
            block = shares[pair * 2 * rows : (pair + 1) * 2 * rows]
            result = jnp.dot(
                jnp.where(pair_mask, block, jnp.zeros_like(block)),
                jnp.concatenate(
                    stacked_values[pair * 2 * HEADS : (pair + 1) * 2 * HEADS], axis=0
                ),
                preferred_element_type=jnp.float32,
            )
            for inner in range(2):
                feat = step * together + pair * 2 + inner
                item_ref[pl.ds(feat, rows, stride=feats), :] = result[
                    inner * rows : (inner + 1) * rows
                ]

    def items(step, carry):
        for inner in range(ITEM_STEP):
            item(step * ITEM_STEP + inner)
        return carry

    lax.fori_loop(0, feats // (together * ITEM_STEP), items, 0)

    def last(step, carry):
        attended = item_ref[span(step), :].astype(jnp.bfloat16)
        update = jnp.dot(attended, item_out[...], preferred_element_type=jnp.float32)
        result = (mixed_ref[span(step), :].astype(jnp.float32) + update).astype(jnp.bfloat16)
        for row in range(step_rows):
            result_ref[step * step_rows + row] = result[row * feats : (row + 1) * feats]
        return carry

    lax.fori_loop(0, rows // step_rows, last, 0)
    copy = pltpu.make_async_copy(result_ref, out_ref.at[pl.ds(first_row, rows)], sem)
    copy.start()
    copy.wait()


ITEM_STEP = 5


def own_rows(parts, feat_qkv, feat_out, item_qkv, item_out, keys, bias, total, first, before):
    feats_here, rows, width = parts[0].shape
    feats = len(parts) * feats_here
    table = pltpu.VMEM((rows * feats, width), jnp.float32)
    block = pl.BlockSpec(memory_space=pltpu.VMEM)
    anywhere = pl.BlockSpec(memory_space=pltpu.HBM)
    aliased = [] if before is None else [before]
    return pl.pallas_call(
        functools.partial(row_kernel, first, len(aliased)),
        out_shape=jax.ShapeDtypeStruct((total, feats, width), jnp.bfloat16),
        in_specs=[block] * (len(parts) + 6) + [anywhere] * len(aliased),
        out_specs=anywhere,
        scratch_shapes=[
            table,
            pltpu.VMEM((rows * feats, width), jnp.bfloat16),
            table,
            table,
            pltpu.VMEM((rows, feats, width), jnp.bfloat16),
            pltpu.SemaphoreType.DMA,
        ],
        input_output_aliases={len(parts) + 6: 0} if aliased else {},
        compiler_params=pltpu.CompilerParams(vmem_limit_bytes=24 << 20),
        name="rows",
    )(*parts, feat_qkv, feat_out, item_qkv, item_out, keys, bias, *aliased)


def swap(tensor, step):
    devices = lax.axis_size("feat")
    return lax.ppermute(tensor, "feat", [(one, one ^ step) for one in range(devices)])


CHUNKS = 2


def one_block_per_table(cells, row_live, row_train, feat_qkv, feat_out, item_qkv, item_out):
    feat_devices = lax.axis_size("feat")
    group_rows = cells.shape[0] // feat_devices
    bias, train_rows, near, sends = prepare(cells, row_live, row_train, CHUNKS)
    near_part = swap(near, 1)
    train_parts = [train_rows, near_part]
    for step in range(2, feat_devices):
        low = step & -step
        if low == step:
            train_parts.append(swap(train_rows, step))
        else:
            train_parts.append(swap(train_parts[step - low], low))
    row_parts = [
        [sends[0][at], near_part]
        + [swap(sends[step][at], step) for step in range(2, feat_devices)]
        for at in range(CHUNKS)
    ]
    keys = key_rows(train_parts, feat_qkv, feat_out, item_qkv)
    result = None
    for at, parts in enumerate(row_parts):
        result = own_rows(
            parts,
            feat_qkv,
            feat_out,
            item_qkv,
            item_out,
            keys,
            bias,
            group_rows,
            at * (group_rows // CHUNKS),
            result,
        )
    return result


def layer(cells, block_table, *rest):
    if block_table.shape[0] == TABLES:
        return one_block_per_table(cells, *rest)
    return on_device(cells, block_table, *rest)


def solution(mesh):
    return jax.shard_map(
        layer,
        mesh=mesh,
        in_specs=(P("rows", "feat", None), P(), P(), P(), P(), P(), P(), P()),
        out_specs=P(("rows", "feat"), None, None),
        check_vma=False,
    )
```

```python
import functools
import math

import jax
import jax.numpy as jnp
from jax import lax
from jax.experimental import pallas as pl
from jax.experimental.pallas import tpu as pltpu
from jax.sharding import PartitionSpec as P

HEADS = 4
HEAD_DIM = 32
KEEP = 4
TABLES = 8


EPSILON = 1e-05
MASKED = -1e30
SCALE2 = HEAD_DIM ** (-0.5) * math.log2(math.e)


def compact_train(train_rows):
    positions = jnp.arange(train_rows.shape[-1], dtype=jnp.int32)
    ordinal = jnp.cumsum(train_rows, axis=-1) - 1
    slot_ids = jnp.arange(KEEP, dtype=jnp.int32)
    matched = (train_rows[..., None, :] == 1) & (ordinal[..., None, :] == slot_ids[:, None])
    return jnp.sum(jnp.where(matched, positions, 0), axis=-1)


def into_heads(tensor):
    return tensor.reshape(tensor.shape[:-1] + (HEADS, HEAD_DIM))


def attend_features(queries, key_part, value_part):
    row_count, query_feats = (queries.shape[0], queries.shape[1])
    blocks = max(1, row_count * query_feats // 1280)
    while row_count % blocks:
        blocks -= 1
    scaling = HEAD_DIM ** (-0.5)

    def attend_one_block(block_parts):
        block_query, block_key, block_value = block_parts
        scores = (
            jnp.einsum(
                "rqhd,rkhd->rhqk", block_query, block_key, preferred_element_type=jnp.float32
            )
            * scaling
        )
        shares = jax.nn.softmax(scores, axis=-1).astype(jnp.bfloat16)
        return jnp.einsum(
            "rhqk,rkhd->rqhd", shares, block_value, preferred_element_type=jnp.float32
        ).astype(jnp.bfloat16)

    def by_block(tensor):
        return tensor.reshape((blocks, row_count // blocks) + tensor.shape[1:])

    result = lax.map(
        attend_one_block, (by_block(queries), by_block(key_part), by_block(value_part))
    )
    return result.reshape(row_count, query_feats, HEADS * HEAD_DIM)


def feature_layer(normed_cells, feat_out, key_part, value_part, queries):
    attended = attend_features(queries, key_part, value_part)
    update = jnp.dot(attended, feat_out, preferred_element_type=jnp.float32)
    return (normed_cells.astype(jnp.float32) + update).astype(jnp.bfloat16)


def on_device(cells, block_table, row_live, row_train, feat_qkv, feat_out, item_qkv, item_out):
    rows_here, _, width_all = cells.shape
    row_index = lax.axis_index("rows")
    feat_index = lax.axis_index("feat")
    row_devices = lax.axis_size("rows")
    feat_devices = lax.axis_size("feat")
    my_table = lax.dynamic_index_in_dim(block_table, row_index, keepdims=False)
    live_rows = lax.dynamic_slice_in_dim(row_live, row_index * rows_here, rows_here).astype(
        jnp.float32
    )
    values = cells.astype(jnp.float32)
    table_hot = (jnp.arange(TABLES, dtype=jnp.int32) == my_table).astype(jnp.float32)
    first_local = jnp.sum(values * live_rows[:, None, None], axis=(0, 2))
    count_local = jnp.sum(live_rows) * width_all
    first_sum, count_sum = lax.psum(
        (table_hot[:, None] * first_local[None, :], table_hot * count_local), "rows"
    )
    table_mean = first_sum / count_sum[:, None]
    mine_mean = lax.dynamic_index_in_dim(table_mean, my_table, keepdims=False)
    centred = values - mine_mean[None, :, None]
    second_local = jnp.sum(centred * centred * live_rows[:, None, None], axis=(0, 2))
    second_sum = lax.psum(table_hot[:, None] * second_local[None, :], "rows")
    table_spread = second_sum / count_sum[:, None]
    mine_spread = lax.dynamic_index_in_dim(table_spread, my_table, keepdims=False)
    normed = (centred * lax.rsqrt(mine_spread + EPSILON)[None, :, None]).astype(jnp.bfloat16)
    normed_rows = lax.all_to_all(normed, "feat", split_axis=0, concat_axis=1, tiled=True)
    projected = jnp.dot(normed_rows, feat_qkv, preferred_element_type=jnp.float32).astype(
        jnp.bfloat16
    )
    queries = into_heads(projected[..., :width_all])
    key_part = into_heads(projected[..., width_all : 2 * width_all])
    value_part = into_heads(projected[..., 2 * width_all :])
    mixed_rows = feature_layer(normed_rows, feat_out, key_part, value_part, queries)
    group_rows, total_feats = (mixed_rows.shape[0], mixed_rows.shape[1])
    per_device = total_feats * HEADS // row_devices
    first_row = row_index * rows_here + feat_index * group_rows
    train_here = lax.dynamic_slice_in_dim(row_train, first_row, group_rows)
    places = compact_train(train_here)
    chosen = jnp.take(mixed_rows, places, axis=0)
    item_query = jnp.dot(
        mixed_rows, item_qkv[:, :width_all], preferred_element_type=jnp.float32
    ).astype(jnp.bfloat16)
    item_query = item_query.reshape(group_rows, row_devices, per_device, HEAD_DIM)
    key_value = jnp.dot(chosen, item_qkv[:, width_all:], preferred_element_type=jnp.float32).astype(
        jnp.bfloat16
    )
    item_key = key_value[..., :width_all].reshape(KEEP, row_devices, per_device, HEAD_DIM)
    item_value = key_value[..., width_all:].reshape(KEEP, row_devices, per_device, HEAD_DIM)
    query_table = jnp.repeat(block_table, group_rows)
    groups_all = row_train.reshape(row_devices, feat_devices, group_rows)
    group_counts = jnp.sum(groups_all, axis=2)
    slot_ids = jnp.arange(KEEP, dtype=jnp.int32)
    key_valid = slot_ids[None, None, :] < jnp.transpose(group_counts)[:, :, None]
    key_table = jnp.broadcast_to(block_table[None, :, None], key_valid.shape)
    allowed = (query_table[:, None] == key_table.reshape(-1)[None, :]) & key_valid.reshape(-1)[
        None, :
    ]
    query_count = query_table.shape[0]
    key_count = allowed.shape[1]
    query_blocks = max(1, query_count // 512)
    while query_count % query_blocks:
        query_blocks -= 1
    scaling = HEAD_DIM ** (-0.5)
    blocked_allowed = allowed.reshape(query_blocks, query_count // query_blocks, key_count)
    local_query = lax.all_to_all(item_query, "rows", split_axis=1, concat_axis=0, tiled=True)
    local_key = lax.all_to_all(item_key, "rows", split_axis=1, concat_axis=0, tiled=True)
    local_value = lax.all_to_all(item_value, "rows", split_axis=1, concat_axis=0, tiled=True)
    every_key = lax.all_gather(local_key, "feat", axis=0, tiled=True)
    every_value = lax.all_gather(local_value, "feat", axis=0, tiled=True)

    def one_item(item_parts):
        single_query, single_key, single_value = item_parts

        def one_one_block(block_parts):
            block_query, block_allowed = block_parts
            scores = (
                jnp.dot(block_query, single_key.T, preferred_element_type=jnp.float32) * scaling
            )
            scores = jnp.where(block_allowed, scores, MASKED)
            shares = jax.nn.softmax(scores, axis=-1).astype(jnp.bfloat16)
            return jnp.dot(shares, single_value, preferred_element_type=jnp.float32).astype(
                jnp.bfloat16
            )

        blocked_query = single_query.reshape(query_blocks, query_count // query_blocks, HEAD_DIM)
        return lax.map(one_one_block, (blocked_query, blocked_allowed)).reshape(
            query_count, HEAD_DIM
        )

    by_item = (
        jnp.moveaxis(local_query[:, 0], 1, 0),
        jnp.moveaxis(every_key[:, 0], 1, 0),
        jnp.moveaxis(every_value[:, 0], 1, 0),
    )
    result = jnp.moveaxis(lax.map(one_item, by_item), 0, 1)[:, None]
    attended = lax.all_to_all(result, "rows", split_axis=0, concat_axis=1, tiled=True)
    attended = attended.reshape(group_rows, total_feats, width_all)
    update = jnp.dot(attended, item_out, preferred_element_type=jnp.float32)
    return (mixed_rows.astype(jnp.float32) + update).astype(jnp.bfloat16)


def vmem_kernel(body, shapes, count, scratch, limit):
    many = isinstance(shapes, list)
    block = pl.BlockSpec(memory_space=pltpu.VMEM)
    return pl.pallas_call(
        body,
        out_shape=shapes,
        in_specs=[block] * count,
        out_specs=[block] * len(shapes) if many else block,
        scratch_shapes=scratch,
        compiler_params=pltpu.CompilerParams(vmem_limit_bytes=limit << 20),
    )


PIECES = 4


def prepare_kernel(chunks, live_in, train_in, cells_in, bias_ref, train_out, *refs):
    outs, (live_ref, train_ref, cells_ref, sems) = refs[:-4], refs[-4:]
    feats_here, rows_here, width = cells_ref.shape
    feat_devices = lax.axis_size("feat")
    group_rows = rows_here // feat_devices
    feat_index = lax.axis_index("feat")
    row_index = lax.axis_index("rows")
    keys = train_out.shape[1]
    piece = feats_here // math.gcd(feats_here, PIECES)

    copies = [
        pltpu.make_async_copy(live_in, live_ref, sems.at[0]),
        pltpu.make_async_copy(train_in, train_ref, sems.at[1]),
    ]
    for at, feat in enumerate(range(0, feats_here, piece)):
        here = pl.ds(feat, piece)
        copies.append(
            pltpu.make_async_copy(cells_in.at[here], cells_ref.at[here], sems.at[2 + at])
        )
    for copy in copies:
        copy.start()
    for copy in copies[:2]:
        copy.wait()

    live = live_ref[pl.ds(row_index, 1), :].astype(jnp.float32)
    count = jnp.sum(live, axis=1, keepdims=True) * width
    weight = jnp.transpose(jnp.broadcast_to(live, (width, rows_here)))

    train = jnp.broadcast_to(train_ref[pl.ds(row_index, 1), :], (keys, rows_here))
    before = lax.broadcasted_iota(jnp.int32, (rows_here, rows_here), 0)
    after = lax.broadcasted_iota(jnp.int32, (rows_here, rows_here), 1)
    ladder = (before <= after) & (before // group_rows == after // group_rows)
    ordinal = jnp.dot(
        train.astype(jnp.float32).astype(jnp.bfloat16),
        jnp.where(ladder, 1.0, 0.0).astype(jnp.bfloat16),
        preferred_element_type=jnp.float32,
    )
    key = lax.broadcasted_iota(jnp.int32, (keys, rows_here), 0)
    row = lax.broadcasted_iota(jnp.int32, (keys, rows_here), 1)
    here = (
        (train == 1)
        & (row // group_rows == key // KEEP)
        & (ordinal == (key % KEEP + 1).astype(jnp.float32))
    )
    chosen = jnp.where(here, 1.0, 0.0)
    found = jnp.sum(chosen, axis=1, keepdims=True)
    bias_ref[...] = jnp.broadcast_to(jnp.where(found > 0.5, 0.0, MASKED), bias_ref.shape)
    picks = jnp.concatenate(
        [chosen, jnp.broadcast_to(live, (keys, rows_here))], axis=0
    ).astype(jnp.bfloat16)

    means, train_rows = [], []
    for feat in range(feats_here):
        if feat % piece == 0:
            copies[2 + feat // piece].wait()
        picked = jnp.dot(picks, cells_ref[feat], preferred_element_type=jnp.float32)
        train_rows.append(picked[:keys])
        total = jnp.sum(picked[keys : keys + 1], axis=1, keepdims=True)
        means.append(jnp.broadcast_to(total / count, (1, width)))
    factors = []
    for feat in range(feats_here):
        centred = cells_ref[feat].astype(jnp.float32) - means[feat]
        total = jnp.sum(centred * centred * weight, axis=0, keepdims=True)
        spread = jnp.sum(total, axis=1, keepdims=True) / count
        factors.append(jnp.broadcast_to(lax.rsqrt(spread + EPSILON), (1, width)))

    def normed(feat, values):
        centred = values.astype(jnp.float32) - means[feat]
        return (centred * factors[feat]).astype(jnp.bfloat16)

    near_out = outs[0]
    for feat in range(feats_here):
        rows = normed(feat, train_rows[feat])
        train_out[feat] = rows
        near_out[0, feat] = rows
    for step in range(feat_devices):
        for at in range(chunks):
            size = group_rows // chunks
            first_row = pl.multiple_of((feat_index ^ step) * group_rows + at * size, size)
            for feat in range(feats_here):
                rows = normed(feat, cells_ref[feat, pl.ds(first_row, size), :])
                if step == 1:
                    near_out[1 + at, feat] = rows
                else:
                    outs[1 + max(step - 1, 0) * chunks + at][feat] = rows


def prepare(cells, row_live, row_train, chunks):
    rows_here, feats_here, width = cells.shape
    feat_devices = lax.axis_size("feat")
    keys = feat_devices * KEEP
    shapes = [
        jax.ShapeDtypeStruct((keys, 128), jnp.float32),
        jax.ShapeDtypeStruct((feats_here, keys, width), jnp.bfloat16),
    ]
    size = rows_here // feat_devices // chunks
    assert size == keys
    part = jax.ShapeDtypeStruct((feats_here, size, width), jnp.bfloat16)
    shapes.append(jax.ShapeDtypeStruct((1 + chunks,) + part.shape, jnp.bfloat16))
    shapes += [part] * ((feat_devices - 1) * chunks)
    blocks = row_live.shape[0] // rows_here
    block = pl.BlockSpec(memory_space=pltpu.VMEM)
    outs = pl.pallas_call(
        functools.partial(prepare_kernel, chunks),
        out_shape=shapes,
        in_specs=[pl.BlockSpec(memory_space=pltpu.HBM)] * 3,
        out_specs=[block] * len(shapes),
        scratch_shapes=[
            pltpu.VMEM((blocks, rows_here), jnp.int32),
            pltpu.VMEM((blocks, rows_here), jnp.int32),
            pltpu.VMEM((feats_here, rows_here, width), jnp.bfloat16),
            pltpu.SemaphoreType.DMA((2 + math.gcd(feats_here, PIECES),)),
        ],
        compiler_params=pltpu.CompilerParams(vmem_limit_bytes=8 << 20),
        name="prepare",
    )(
        pltpu.with_memory_space_constraint(row_live.reshape(-1, rows_here), pltpu.HBM),
        pltpu.with_memory_space_constraint(row_train.reshape(-1, rows_here), pltpu.HBM),
        pltpu.with_memory_space_constraint(jnp.transpose(cells, (1, 0, 2)), pltpu.HBM),
    )
    sends = {
        step: outs[3 + at * chunks : 3 + (at + 1) * chunks]
        for at, step in enumerate([0, *range(2, feat_devices)])
    }
    return outs[0], outs[1], outs[2], sends


def pitch(count):
    return count + 4 if count % 8 == 0 else count


def gather_parts(parts, at, held):
    feat_index = lax.axis_index("feat")
    feats_here, rows, _ = parts[0].shape
    for step, part in enumerate(parts):
        first = (feat_index ^ step) * (feats_here * pitch(rows))
        values = part[at] if step == 1 else part[...]
        for feat in range(feats_here):
            held[pl.ds(first + feat * pitch(rows), rows), :] = values[feat].astype(jnp.float32)


def head_masks(rows, width):
    lane = lax.broadcasted_iota(jnp.int32, (rows, width), 1)
    return [(lane // HEAD_DIM) == head for head in range(HEADS)]


def by_head(tensor, masks):
    return [jnp.where(mask, tensor, jnp.zeros_like(tensor)) for mask in masks]


def attend(queries, keys, values, masks):
    count = queries.shape[0]
    scores = lax.dot_general(
        jnp.concatenate(by_head(keys, masks), axis=0),
        queries,
        (((1,), (1,)), ((), ())),
        preferred_element_type=jnp.float32,
    ).reshape(HEADS, count, count)
    top = jnp.max(scores, axis=1, keepdims=True)
    powers = jnp.exp2((scores - top) * SCALE2)
    shares = powers * (1.0 / jnp.sum(powers, axis=1, keepdims=True))
    shares = shares.reshape(HEADS * count, count).astype(jnp.bfloat16)
    return lax.dot_general(
        shares,
        jnp.concatenate(by_head(values, masks), axis=0),
        (((0,), (0,)), ((), ())),
        preferred_element_type=jnp.float32,
    )


def feature_rows(held, mixed_ref, rows, qkv_ref, out_ref):
    feats, width = held.shape[0] // pitch(rows), held.shape[1]
    cells = [held[pl.ds(row, feats, stride=pitch(rows)), :] for row in range(rows)]
    projected = jnp.dot(
        jnp.concatenate(cells, axis=0).astype(jnp.bfloat16),
        qkv_ref[...],
        preferred_element_type=jnp.float32,
    ).astype(jnp.bfloat16)
    masks = head_masks(feats, width)
    attended = []
    for row in range(rows):
        block = projected[row * feats : (row + 1) * feats]
        attended.append(
            attend(
                block[:, :width],
                block[:, width : 2 * width],
                block[:, 2 * width :],
                masks,
            ).astype(jnp.bfloat16)
        )
    update = jnp.dot(
        jnp.concatenate(attended, axis=0), out_ref[...], preferred_element_type=jnp.float32
    )
    for row in range(rows):
        mixed = (cells[row] + update[row * feats : (row + 1) * feats]).astype(jnp.bfloat16)
        mixed_ref[pl.ds(row * pitch(feats), feats), :] = mixed.astype(jnp.float32)


def by_feature(mixed_ref, first, count, rows, stride):
    return jnp.concatenate(
        [mixed_ref[pl.ds(first + feat, rows, stride=stride), :] for feat in range(count)], axis=0
    )


def key_kernel(*refs):
    feat_devices = lax.axis_size("feat")
    parts = refs[:feat_devices]
    feat_qkv, feat_out, item_qkv, out_ref, held, mixed_ref = refs[feat_devices:]
    feats, rows, width = out_ref.shape[0], out_ref.shape[1], held.shape[1]
    gather_parts(parts, 0, held)
    feature_rows(held, mixed_ref, rows, feat_qkv, feat_out)
    together = 128 // rows
    for feat in range(0, feats, together):
        mixed = by_feature(mixed_ref, feat, together, rows, pitch(feats)).astype(jnp.bfloat16)
        both = jnp.dot(mixed, item_qkv[:, width:], preferred_element_type=jnp.float32)
        out_ref[pl.ds(feat, together)] = both.astype(jnp.bfloat16).reshape(
            together, rows, 2 * width
        )


def key_rows(parts, feat_qkv, feat_out, item_qkv):
    feats_here, rows, width = parts[0].shape
    feats = len(parts) * feats_here
    return vmem_kernel(
        key_kernel,
        jax.ShapeDtypeStruct((feats, rows, 2 * width), jnp.bfloat16),
        len(parts) + 3,
        [
            pltpu.VMEM((feats * pitch(rows), width), jnp.float32),
            pltpu.VMEM((rows * pitch(feats), width), jnp.float32),
        ],
        24,
    )(*parts, feat_qkv, feat_out, item_qkv)


def row_kernel(first_row, earlier, last, *refs):
    feat_devices = lax.axis_size("feat")
    parts = refs[:feat_devices]
    (feat_qkv, feat_out, item_qkv, item_out, keys_ref, bias_ref) = refs[
        feat_devices : feat_devices + 6
    ]
    results = refs[feat_devices + 6 : feat_devices + 6 + earlier]
    out_ref, held, mixed_ref, query_ref, item_ref, total_ref, *own = refs[
        feat_devices + 6 + earlier :
    ]
    rows, width = parts[0].shape[1], held.shape[1]
    feats, keys = keys_ref.shape[0], keys_ref.shape[1]
    copies = []

    def send(source, at, count):
        copy = pltpu.make_async_copy(source, out_ref.at[pl.ds(at, count)], own[1].at[len(copies)])
        copy.start()
        copies.append(copy)

    for at, result in enumerate(results):
        send(result, at * rows, rows)
    gather_parts(parts, 1 + first_row // rows, held)
    feature_rows(held, mixed_ref, rows, feat_qkv, feat_out)

    stride = pitch(feats)
    together = 128 // rows
    lanes = together * rows
    size = HEADS * keys
    key_masks = head_masks(keys, width)
    bias = jnp.concatenate([bias_ref[:, :lanes]] * HEADS, axis=0)
    lane_owner = lax.broadcasted_iota(jnp.int32, (size, lanes), 1) // rows
    pair_row = lax.broadcasted_iota(jnp.int32, (2 * rows, 2 * size), 0) // rows
    pair_lane = lax.broadcasted_iota(jnp.int32, (2 * rows, 2 * size), 1) // size
    pair_mask = pair_row == pair_lane

    for first in range(0, feats, together):
        mixed = by_feature(mixed_ref, first, together, rows, stride)
        query_ref[pl.ds(first * rows, lanes), :] = jnp.dot(
            mixed.astype(jnp.bfloat16), item_qkv[:, :width], preferred_element_type=jnp.float32
        ).astype(jnp.bfloat16)

    def item(first):
        stacked_keys, stacked_values = [], []
        for inner in range(together):
            stacked_keys += by_head(keys_ref[first + inner, :, :width], key_masks)
            stacked_values += by_head(keys_ref[first + inner, :, width:], key_masks)
        every = lax.dot_general(
            jnp.concatenate(stacked_keys, axis=0),
            query_ref[pl.ds(pl.multiple_of(first * rows, lanes), lanes), :],
            (((1,), (1,)), ((), ())),
            preferred_element_type=jnp.float32,
        )
        scores = every[:size]
        for inner in range(1, together):
            scores = jnp.where(lane_owner == inner, every[inner * size : (inner + 1) * size], scores)
        scores = (scores + bias).reshape(HEADS, keys, lanes)
        top = jnp.max(scores, axis=1, keepdims=True)
        powers = jnp.exp2((scores - top) * SCALE2)
        shares = powers * (1.0 / jnp.sum(powers, axis=1, keepdims=True))
        shares = shares.reshape(size, lanes)
        shares = jnp.transpose(jnp.concatenate([shares, shares], axis=0)).astype(jnp.bfloat16)
        for pair in range(together // 2):
            block = shares[pair * 2 * rows : (pair + 1) * 2 * rows]
            here = pl.multiple_of((first + pair * 2) * rows, 2 * rows)
            item_ref[pl.ds(here, 2 * rows), :] = jnp.dot(
                jnp.where(pair_mask, block, jnp.zeros_like(block)),
                jnp.concatenate(
                    stacked_values[pair * 2 * HEADS : (pair + 1) * 2 * HEADS], axis=0
                ),
                preferred_element_type=jnp.float32,
            ).astype(jnp.bfloat16)

    def items(step, carry):
        for inner in range(ITEM_STEP):
            item((step * ITEM_STEP + inner) * together)
        return carry

    lax.fori_loop(0, feats // (together * ITEM_STEP), items, 0)
    for first in range(0, feats, together):
        update = jnp.dot(
            item_ref[pl.ds(first * rows, lanes), :],
            item_out[...],
            preferred_element_type=jnp.float32,
        )
        total = by_feature(mixed_ref, first, together, rows, stride) + update
        for inner in range(together):
            total_ref[pl.ds(first + inner, rows, stride=stride), :] = total[
                inner * rows : (inner + 1) * rows
            ]
    result_ref = own[0] if last else out_ref
    for row in range(rows):
        result_ref[row] = total_ref[pl.ds(row * stride, feats), :].astype(jnp.bfloat16)
        if last and (row + 1) % OUT_ROWS == 0:
            first = row + 1 - OUT_ROWS
            send(result_ref.at[pl.ds(first, OUT_ROWS)], first_row + first, OUT_ROWS)
    for copy in copies:
        copy.wait()


OUT_ROWS = 4
ITEM_STEP = 10


def own_rows(parts, feat_qkv, feat_out, item_qkv, item_out, keys, bias, total, first, results):
    feats_here, rows, width = parts[0].shape
    feats = len(parts) * feats_here
    last = first + rows == total
    results = results if last else []
    table = pltpu.VMEM((rows * pitch(feats), width), jnp.float32)
    packed = pltpu.VMEM((rows * feats, width), jnp.bfloat16)
    scratch = [pltpu.VMEM((feats * pitch(rows), width), jnp.float32), table, packed, packed, table]
    if last:
        scratch.append(pltpu.VMEM((rows, feats, width), jnp.bfloat16))
        scratch.append(pltpu.SemaphoreType.DMA((len(results) + rows // OUT_ROWS,)))
    block = pl.BlockSpec(memory_space=pltpu.VMEM)
    return pl.pallas_call(
        functools.partial(row_kernel, first, len(results), last),
        out_shape=jax.ShapeDtypeStruct((total if last else rows, feats, width), jnp.bfloat16),
        in_specs=[block] * (len(parts) + 6 + len(results)),
        out_specs=pl.BlockSpec(memory_space=pltpu.HBM) if last else block,
        scratch_shapes=scratch,
        compiler_params=pltpu.CompilerParams(vmem_limit_bytes=24 << 20),
        name="rows",
    )(*parts, feat_qkv, feat_out, item_qkv, item_out, keys, bias, *results)


def swap(tensor, step):
    devices = lax.axis_size("feat")
    return lax.ppermute(tensor, "feat", [(one, one ^ step) for one in range(devices)])


CHUNKS = 2


def one_block_per_table(cells, row_live, row_train, feat_qkv, feat_out, item_qkv, item_out):
    feat_devices = lax.axis_size("feat")
    group_rows = cells.shape[0] // feat_devices
    bias, train_rows, near, sends = prepare(cells, row_live, row_train, CHUNKS)
    near_part = swap(near, 1)
    train_parts = [train_rows, near_part]
    for step in range(2, feat_devices):
        low = step & -step
        if low == step:
            train_parts.append(swap(train_rows, step))
        else:
            train_parts.append(swap(train_parts[step - low], low))
    row_parts = [
        [sends[0][at], near_part]
        + [swap(sends[step][at], step) for step in range(2, feat_devices)]
        for at in range(CHUNKS)
    ]
    keys = key_rows(train_parts, feat_qkv, feat_out, item_qkv)
    results = []
    for at, parts in enumerate(row_parts):
        result = own_rows(
            parts,
            feat_qkv,
            feat_out,
            item_qkv,
            item_out,
            keys,
            bias,
            group_rows,
            at * (group_rows // CHUNKS),
            results,
        )
        results.append(result)
    return results[-1]


def layer(cells, block_table, *rest):
    if block_table.shape[0] == TABLES:
        return one_block_per_table(cells, *rest)
    return on_device(cells, block_table, *rest)


def solution(mesh):
    return jax.shard_map(
        layer,
        mesh=mesh,
        in_specs=(P("rows", "feat", None), P(), P(), P(), P(), P(), P(), P()),
        out_specs=P(("rows", "feat"), None, None),
        check_vma=False,
    )
```

```python
import functools
import math

import jax
import jax.numpy as jnp
from jax import lax
from jax.experimental import pallas as pl
from jax.experimental.pallas import tpu as pltpu
from jax.sharding import PartitionSpec as P

HEADS = 4
HEAD_DIM = 32
KEEP = 4
TABLES = 8


EPSILON = 1e-05
MASKED = -1e30
SCALE2 = HEAD_DIM ** (-0.5) * math.log2(math.e)


def compact_train(train_rows):
    positions = jnp.arange(train_rows.shape[-1], dtype=jnp.int32)
    ordinal = jnp.cumsum(train_rows, axis=-1) - 1
    slot_ids = jnp.arange(KEEP, dtype=jnp.int32)
    matched = (train_rows[..., None, :] == 1) & (ordinal[..., None, :] == slot_ids[:, None])
    return jnp.sum(jnp.where(matched, positions, 0), axis=-1)


def into_heads(tensor):
    return tensor.reshape(tensor.shape[:-1] + (HEADS, HEAD_DIM))


def attend_features(queries, key_part, value_part):
    row_count, query_feats = (queries.shape[0], queries.shape[1])
    blocks = max(1, row_count * query_feats // 1280)
    while row_count % blocks:
        blocks -= 1
    scaling = HEAD_DIM ** (-0.5)

    def attend_one_block(block_parts):
        block_query, block_key, block_value = block_parts
        scores = (
            jnp.einsum(
                "rqhd,rkhd->rhqk", block_query, block_key, preferred_element_type=jnp.float32
            )
            * scaling
        )
        shares = jax.nn.softmax(scores, axis=-1).astype(jnp.bfloat16)
        return jnp.einsum(
            "rhqk,rkhd->rqhd", shares, block_value, preferred_element_type=jnp.float32
        ).astype(jnp.bfloat16)

    def by_block(tensor):
        return tensor.reshape((blocks, row_count // blocks) + tensor.shape[1:])

    result = lax.map(
        attend_one_block, (by_block(queries), by_block(key_part), by_block(value_part))
    )
    return result.reshape(row_count, query_feats, HEADS * HEAD_DIM)


def feature_layer(normed_cells, feat_out, key_part, value_part, queries):
    attended = attend_features(queries, key_part, value_part)
    update = jnp.dot(attended, feat_out, preferred_element_type=jnp.float32)
    return (normed_cells.astype(jnp.float32) + update).astype(jnp.bfloat16)


def on_device(cells, block_table, row_live, row_train, feat_qkv, feat_out, item_qkv, item_out):
    rows_here, _, width_all = cells.shape
    row_index = lax.axis_index("rows")
    feat_index = lax.axis_index("feat")
    row_devices = lax.axis_size("rows")
    feat_devices = lax.axis_size("feat")
    my_table = lax.dynamic_index_in_dim(block_table, row_index, keepdims=False)
    live_rows = lax.dynamic_slice_in_dim(row_live, row_index * rows_here, rows_here).astype(
        jnp.float32
    )
    values = cells.astype(jnp.float32)
    table_hot = (jnp.arange(TABLES, dtype=jnp.int32) == my_table).astype(jnp.float32)
    first_local = jnp.sum(values * live_rows[:, None, None], axis=(0, 2))
    count_local = jnp.sum(live_rows) * width_all
    first_sum, count_sum = lax.psum(
        (table_hot[:, None] * first_local[None, :], table_hot * count_local), "rows"
    )
    table_mean = first_sum / count_sum[:, None]
    mine_mean = lax.dynamic_index_in_dim(table_mean, my_table, keepdims=False)
    centred = values - mine_mean[None, :, None]
    second_local = jnp.sum(centred * centred * live_rows[:, None, None], axis=(0, 2))
    second_sum = lax.psum(table_hot[:, None] * second_local[None, :], "rows")
    table_spread = second_sum / count_sum[:, None]
    mine_spread = lax.dynamic_index_in_dim(table_spread, my_table, keepdims=False)
    normed = (centred * lax.rsqrt(mine_spread + EPSILON)[None, :, None]).astype(jnp.bfloat16)
    normed_rows = lax.all_to_all(normed, "feat", split_axis=0, concat_axis=1, tiled=True)
    projected = jnp.dot(normed_rows, feat_qkv, preferred_element_type=jnp.float32).astype(
        jnp.bfloat16
    )
    queries = into_heads(projected[..., :width_all])
    key_part = into_heads(projected[..., width_all : 2 * width_all])
    value_part = into_heads(projected[..., 2 * width_all :])
    mixed_rows = feature_layer(normed_rows, feat_out, key_part, value_part, queries)
    group_rows, total_feats = (mixed_rows.shape[0], mixed_rows.shape[1])
    per_device = total_feats * HEADS // row_devices
    first_row = row_index * rows_here + feat_index * group_rows
    train_here = lax.dynamic_slice_in_dim(row_train, first_row, group_rows)
    places = compact_train(train_here)
    chosen = jnp.take(mixed_rows, places, axis=0)
    item_query = jnp.dot(
        mixed_rows, item_qkv[:, :width_all], preferred_element_type=jnp.float32
    ).astype(jnp.bfloat16)
    item_query = item_query.reshape(group_rows, row_devices, per_device, HEAD_DIM)
    key_value = jnp.dot(chosen, item_qkv[:, width_all:], preferred_element_type=jnp.float32).astype(
        jnp.bfloat16
    )
    item_key = key_value[..., :width_all].reshape(KEEP, row_devices, per_device, HEAD_DIM)
    item_value = key_value[..., width_all:].reshape(KEEP, row_devices, per_device, HEAD_DIM)
    query_table = jnp.repeat(block_table, group_rows)
    groups_all = row_train.reshape(row_devices, feat_devices, group_rows)
    group_counts = jnp.sum(groups_all, axis=2)
    slot_ids = jnp.arange(KEEP, dtype=jnp.int32)
    key_valid = slot_ids[None, None, :] < jnp.transpose(group_counts)[:, :, None]
    key_table = jnp.broadcast_to(block_table[None, :, None], key_valid.shape)
    allowed = (query_table[:, None] == key_table.reshape(-1)[None, :]) & key_valid.reshape(-1)[
        None, :
    ]
    query_count = query_table.shape[0]
    key_count = allowed.shape[1]
    query_blocks = max(1, query_count // 512)
    while query_count % query_blocks:
        query_blocks -= 1
    scaling = HEAD_DIM ** (-0.5)
    blocked_allowed = allowed.reshape(query_blocks, query_count // query_blocks, key_count)
    local_query = lax.all_to_all(item_query, "rows", split_axis=1, concat_axis=0, tiled=True)
    local_key = lax.all_to_all(item_key, "rows", split_axis=1, concat_axis=0, tiled=True)
    local_value = lax.all_to_all(item_value, "rows", split_axis=1, concat_axis=0, tiled=True)
    every_key = lax.all_gather(local_key, "feat", axis=0, tiled=True)
    every_value = lax.all_gather(local_value, "feat", axis=0, tiled=True)

    def one_item(item_parts):
        single_query, single_key, single_value = item_parts

        def one_one_block(block_parts):
            block_query, block_allowed = block_parts
            scores = (
                jnp.dot(block_query, single_key.T, preferred_element_type=jnp.float32) * scaling
            )
            scores = jnp.where(block_allowed, scores, MASKED)
            shares = jax.nn.softmax(scores, axis=-1).astype(jnp.bfloat16)
            return jnp.dot(shares, single_value, preferred_element_type=jnp.float32).astype(
                jnp.bfloat16
            )

        blocked_query = single_query.reshape(query_blocks, query_count // query_blocks, HEAD_DIM)
        return lax.map(one_one_block, (blocked_query, blocked_allowed)).reshape(
            query_count, HEAD_DIM
        )

    by_item = (
        jnp.moveaxis(local_query[:, 0], 1, 0),
        jnp.moveaxis(every_key[:, 0], 1, 0),
        jnp.moveaxis(every_value[:, 0], 1, 0),
    )
    result = jnp.moveaxis(lax.map(one_item, by_item), 0, 1)[:, None]
    attended = lax.all_to_all(result, "rows", split_axis=0, concat_axis=1, tiled=True)
    attended = attended.reshape(group_rows, total_feats, width_all)
    update = jnp.dot(attended, item_out, preferred_element_type=jnp.float32)
    return (mixed_rows.astype(jnp.float32) + update).astype(jnp.bfloat16)


def vmem_kernel(body, shapes, count, scratch, limit):
    many = isinstance(shapes, list)
    block = pl.BlockSpec(memory_space=pltpu.VMEM)
    return pl.pallas_call(
        body,
        out_shape=shapes,
        in_specs=[block] * count,
        out_specs=[block] * len(shapes) if many else block,
        scratch_shapes=scratch,
        compiler_params=pltpu.CompilerParams(vmem_limit_bytes=limit << 20),
    )


PIECES = 1


def prepare_kernel(chunks, live_in, train_in, cells_in, bias_ref, train_out, *refs):
    outs, (live_ref, train_ref, cells_ref, sems) = refs[:-4], refs[-4:]
    feats_here, rows_here, width = cells_ref.shape
    feat_devices = lax.axis_size("feat")
    group_rows = rows_here // feat_devices
    feat_index = lax.axis_index("feat")
    row_index = lax.axis_index("rows")
    keys = train_out.shape[1]
    piece = feats_here // math.gcd(feats_here, PIECES)

    copies = [
        pltpu.make_async_copy(live_in, live_ref, sems.at[0]),
        pltpu.make_async_copy(train_in, train_ref, sems.at[1]),
    ]
    for at, feat in enumerate(range(0, feats_here, piece)):
        here = pl.ds(feat, piece)
        copies.append(
            pltpu.make_async_copy(cells_in.at[here], cells_ref.at[here], sems.at[2 + at])
        )
    for copy in copies:
        copy.start()
    for copy in copies[:2]:
        copy.wait()

    live = live_ref[pl.ds(row_index, 1), :].astype(jnp.float32)
    count = jnp.sum(live, axis=1, keepdims=True) * width
    weight = jnp.transpose(jnp.broadcast_to(live, (width, rows_here)))

    train = jnp.broadcast_to(train_ref[pl.ds(row_index, 1), :], (keys, rows_here))
    before = lax.broadcasted_iota(jnp.int32, (rows_here, rows_here), 0)
    after = lax.broadcasted_iota(jnp.int32, (rows_here, rows_here), 1)
    ladder = (before <= after) & (before // group_rows == after // group_rows)
    ordinal = jnp.dot(
        train.astype(jnp.float32).astype(jnp.bfloat16),
        jnp.where(ladder, 1.0, 0.0).astype(jnp.bfloat16),
        preferred_element_type=jnp.float32,
    )
    key = lax.broadcasted_iota(jnp.int32, (keys, rows_here), 0)
    row = lax.broadcasted_iota(jnp.int32, (keys, rows_here), 1)
    here = (
        (train == 1)
        & (row // group_rows == key // KEEP)
        & (ordinal == (key % KEEP + 1).astype(jnp.float32))
    )
    chosen = jnp.where(here, 1.0, 0.0)
    found = jnp.sum(chosen, axis=1, keepdims=True)
    bias_ref[...] = jnp.broadcast_to(jnp.where(found > 0.5, 0.0, MASKED), bias_ref.shape)
    picks = jnp.concatenate(
        [chosen, jnp.broadcast_to(live, (keys, rows_here))], axis=0
    ).astype(jnp.bfloat16)

    means, train_rows = [], []
    for feat in range(feats_here):
        if feat % piece == 0:
            copies[2 + feat // piece].wait()
        picked = jnp.dot(picks, cells_ref[feat], preferred_element_type=jnp.float32)
        train_rows.append(picked[:keys])
        total = jnp.sum(picked[keys : keys + 1], axis=1, keepdims=True)
        means.append(jnp.broadcast_to(total / count, (1, width)))
    factors = []
    for feat in range(feats_here):
        centred = cells_ref[feat].astype(jnp.float32) - means[feat]
        total = jnp.sum(centred * centred * weight, axis=0, keepdims=True)
        spread = jnp.sum(total, axis=1, keepdims=True) / count
        factors.append(jnp.broadcast_to(lax.rsqrt(spread + EPSILON), (1, width)))

    def normed(feat, values):
        centred = values.astype(jnp.float32) - means[feat]
        return (centred * factors[feat]).astype(jnp.bfloat16)

    near_out = outs[0]
    for feat in range(feats_here):
        rows = normed(feat, train_rows[feat])
        train_out[feat] = rows
        near_out[0, feat] = rows
    for step in range(feat_devices):
        for at in range(chunks):
            size = group_rows // chunks
            first_row = pl.multiple_of((feat_index ^ step) * group_rows + at * size, size)
            for feat in range(feats_here):
                rows = normed(feat, cells_ref[feat, pl.ds(first_row, size), :])
                if step == 1:
                    near_out[1 + at, feat] = rows
                else:
                    outs[1 + max(step - 1, 0) * chunks + at][feat] = rows


def prepare(cells, row_live, row_train, chunks):
    rows_here, feats_here, width = cells.shape
    feat_devices = lax.axis_size("feat")
    keys = feat_devices * KEEP
    shapes = [
        jax.ShapeDtypeStruct((keys, 128), jnp.float32),
        jax.ShapeDtypeStruct((feats_here, keys, width), jnp.bfloat16),
    ]
    size = rows_here // feat_devices // chunks
    assert size == keys
    part = jax.ShapeDtypeStruct((feats_here, size, width), jnp.bfloat16)
    shapes.append(jax.ShapeDtypeStruct((1 + chunks,) + part.shape, jnp.bfloat16))
    shapes += [part] * ((feat_devices - 1) * chunks)
    blocks = row_live.shape[0] // rows_here
    block = pl.BlockSpec(memory_space=pltpu.VMEM)
    outs = pl.pallas_call(
        functools.partial(prepare_kernel, chunks),
        out_shape=shapes,
        in_specs=[pl.BlockSpec(memory_space=pltpu.HBM)] * 3,
        out_specs=[block] * len(shapes),
        scratch_shapes=[
            pltpu.VMEM((blocks, rows_here), jnp.int32),
            pltpu.VMEM((blocks, rows_here), jnp.int32),
            pltpu.VMEM((feats_here, rows_here, width), jnp.bfloat16),
            pltpu.SemaphoreType.DMA((2 + math.gcd(feats_here, PIECES),)),
        ],
        compiler_params=pltpu.CompilerParams(vmem_limit_bytes=8 << 20),
        name="prepare",
    )(
        pltpu.with_memory_space_constraint(row_live.reshape(-1, rows_here), pltpu.HBM),
        pltpu.with_memory_space_constraint(row_train.reshape(-1, rows_here), pltpu.HBM),
        pltpu.with_memory_space_constraint(jnp.transpose(cells, (1, 0, 2)), pltpu.HBM),
    )
    sends = {
        step: outs[3 + at * chunks : 3 + (at + 1) * chunks]
        for at, step in enumerate([0, *range(2, feat_devices)])
    }
    return outs[0], outs[1], outs[2], sends


def pitch(count):
    return count + 4 if count % 8 == 0 else count


def gather_parts(parts, at, held):
    feat_index = lax.axis_index("feat")
    feats_here, rows, _ = parts[0].shape
    for step, part in enumerate(parts):
        first = (feat_index ^ step) * (feats_here * pitch(rows))
        values = part[at] if step == 1 else part[...]
        for feat in range(feats_here):
            held[pl.ds(first + feat * pitch(rows), rows), :] = values[feat].astype(jnp.float32)


def head_masks(rows, width):
    lane = lax.broadcasted_iota(jnp.int32, (rows, width), 1)
    return [(lane // HEAD_DIM) == head for head in range(HEADS)]


def by_head(tensor, masks):
    return [jnp.where(mask, tensor, jnp.zeros_like(tensor)) for mask in masks]


def staggered(stages, count, lag=1):
    for step in range(count + lag * (len(stages) - 1)):
        for at, stage in enumerate(stages):
            if 0 <= step - at * lag < count:
                stage(step - at * lag)


def over_keys(scores, axis):
    top = jnp.max(scores, axis=axis, keepdims=True)
    powers = jnp.exp2(scores - top)
    return powers * (1.0 / jnp.sum(powers, axis=axis, keepdims=True))


def feature_shares(queries, keys, masks):
    count = queries.shape[0]
    scores = lax.dot_general(
        jnp.concatenate(by_head(keys, masks), axis=0),
        queries,
        (((1,), (1,)), ((), ())),
        preferred_element_type=jnp.float32,
    ).reshape(HEADS, count, count)
    return over_keys(scores, 1).reshape(HEADS * count, count).astype(jnp.bfloat16)


def feature_values(shares, values, masks):
    return lax.dot_general(
        shares,
        jnp.concatenate(by_head(values, masks), axis=0),
        (((0,), (0,)), ((), ())),
        preferred_element_type=jnp.float32,
    ).astype(jnp.bfloat16)


STEP = 4


def feature_rows(held, rows, qkv_ref, out_ref, consume):
    feats, width = held.shape[0] // pitch(rows), held.shape[1]
    masks = head_masks(feats, width)
    size = math.gcd(rows, STEP)
    cells, projected, shares, attended = {}, {}, {}, {}

    def project(group):
        cells[group] = jnp.concatenate(
            [
                held[pl.ds(group * size + row, feats, stride=pitch(rows)), :]
                for row in range(size)
            ],
            axis=0,
        )
        every = jnp.dot(
            cells[group].astype(jnp.bfloat16), qkv_ref[...], preferred_element_type=jnp.float32
        )
        projected[group] = [
            (every[:, :width] * SCALE2).astype(jnp.bfloat16),
            every[:, width : 2 * width].astype(jnp.bfloat16),
            every[:, 2 * width :].astype(jnp.bfloat16),
        ]

    def score(group):
        queries, keys, _ = projected[group]
        shares[group] = [
            feature_shares(
                queries[row * feats : (row + 1) * feats],
                keys[row * feats : (row + 1) * feats],
                masks,
            )
            for row in range(size)
        ]

    def attend(group):
        values = projected.pop(group)[2]
        attended[group] = jnp.concatenate(
            [
                feature_values(part, values[row * feats : (row + 1) * feats], masks)
                for row, part in enumerate(shares.pop(group))
            ],
            axis=0,
        )

    def mix(group):
        update = jnp.dot(
            attended.pop(group), out_ref[...], preferred_element_type=jnp.float32
        )
        consume(group * size, size, (cells.pop(group) + update).astype(jnp.bfloat16))

    staggered([project, score, attend, mix], rows // size, 1)


def put_rows(table, first, count, values):
    feats = values.shape[0] // count
    for row in range(count):
        table[pl.ds((first + row) * pitch(feats), feats), :] = values[
            row * feats : (row + 1) * feats
        ]


def by_feature(mixed_ref, first, count, rows, stride):
    return jnp.concatenate(
        [mixed_ref[pl.ds(first + feat, rows, stride=stride), :] for feat in range(count)], axis=0
    )


def key_kernel(*refs):
    feat_devices = lax.axis_size("feat")
    parts = refs[:feat_devices]
    feat_qkv, feat_out, item_qkv, out_ref, held, key_ref, value_ref = refs[feat_devices:]
    feats, rows, width = out_ref.shape[0], out_ref.shape[1], held.shape[1]
    gather_parts(parts, 0, held)

    def consume(first, count, mixed):
        both = jnp.dot(mixed, item_qkv[:, width:], preferred_element_type=jnp.float32)
        put_rows(key_ref, first, count, both[:, :width])
        put_rows(value_ref, first, count, both[:, width:])

    feature_rows(held, rows, feat_qkv, feat_out, consume)
    for feat in range(feats):
        here = pl.ds(feat, rows, stride=pitch(feats))
        out_ref[feat, :, :width] = key_ref[here, :].astype(jnp.bfloat16)
        out_ref[feat, :, width:] = value_ref[here, :].astype(jnp.bfloat16)


def key_rows(parts, feat_qkv, feat_out, item_qkv):
    feats_here, rows, width = parts[0].shape
    feats = len(parts) * feats_here
    return vmem_kernel(
        key_kernel,
        jax.ShapeDtypeStruct((feats, rows, 2 * width), jnp.bfloat16),
        len(parts) + 3,
        [
            pltpu.VMEM((feats * pitch(rows), width), jnp.float32),
            pltpu.VMEM((rows * pitch(feats), width), jnp.float32),
            pltpu.VMEM((rows * pitch(feats), width), jnp.float32),
        ],
        24,
    )(*parts, feat_qkv, feat_out, item_qkv)


def row_kernel(first_row, earlier, last, *refs):
    feat_devices = lax.axis_size("feat")
    parts = refs[:feat_devices]
    (feat_qkv, feat_out, item_qkv, item_out, keys_ref, bias_ref) = refs[
        feat_devices : feat_devices + 6
    ]
    results = refs[feat_devices + 6 : feat_devices + 6 + earlier]
    out_ref, held, mixed_ref, query_ref, total_ref, *own = refs[
        feat_devices + 6 + earlier :
    ]
    rows, width = parts[0].shape[1], held.shape[1]
    feats, keys = keys_ref.shape[0], keys_ref.shape[1]
    copies = []

    def send(source, at, count):
        copy = pltpu.make_async_copy(source, out_ref.at[pl.ds(at, count)], own[1].at[len(copies)])
        copy.start()
        copies.append(copy)

    for at, result in enumerate(results):
        send(result, at * rows, rows)
    gather_parts(parts, 1 + first_row // rows, held)

    def consume(first, count, mixed):
        put_rows(mixed_ref, first, count, mixed.astype(jnp.float32))
        queries = jnp.dot(mixed, item_qkv[:, :width], preferred_element_type=jnp.float32)
        put_rows(query_ref, first, count, queries * SCALE2)

    feature_rows(held, rows, feat_qkv, feat_out, consume)

    stride = pitch(feats)
    together = 128 // rows
    lanes = together * rows
    size = HEADS * keys
    key_masks = head_masks(keys, width)
    bias = jnp.concatenate([bias_ref[:, :lanes]] * HEADS, axis=0)
    lane_owner = lax.broadcasted_iota(jnp.int32, (size, lanes), 1) // rows
    pair_row = lax.broadcasted_iota(jnp.int32, (2 * rows, 2 * size), 0) // rows
    pair_lane = lax.broadcasted_iota(jnp.int32, (2 * rows, 2 * size), 1) // size
    pair_mask = pair_row == pair_lane

    shares, attended = {}, {}

    def score(group):
        first = group * together
        stacked_keys = []
        for feat in range(first, first + together):
            stacked_keys += by_head(keys_ref[feat, :, :width], key_masks)
        every = lax.dot_general(
            jnp.concatenate(stacked_keys, axis=0),
            by_feature(query_ref, first, together, rows, stride).astype(jnp.bfloat16),
            (((1,), (1,)), ((), ())),
            preferred_element_type=jnp.float32,
        )
        scores = every[:size]
        for inner in range(1, together):
            scores = jnp.where(lane_owner == inner, every[inner * size : (inner + 1) * size], scores)
        part = over_keys((scores + bias).reshape(HEADS, keys, lanes), 1).reshape(size, lanes)
        shares[group] = jnp.transpose(jnp.concatenate([part, part], axis=0)).astype(jnp.bfloat16)

    def attend(group):
        part, results = shares.pop(group), []
        for pair in range(together // 2):
            block = part[pair * 2 * rows : (pair + 1) * 2 * rows]
            stacked_values = []
            for inner in range(2):
                feat = group * together + pair * 2 + inner
                stacked_values += by_head(keys_ref[feat, :, width:], key_masks)
            results.append(
                jnp.dot(
                    jnp.where(pair_mask, block, jnp.zeros_like(block)),
                    jnp.concatenate(stacked_values, axis=0),
                    preferred_element_type=jnp.float32,
                ).astype(jnp.bfloat16)
            )
        attended[group] = jnp.concatenate(results, axis=0)

    def finish(group):
        first = group * together
        update = jnp.dot(attended.pop(group), item_out[...], preferred_element_type=jnp.float32)
        total = by_feature(mixed_ref, first, together, rows, stride) + update
        for inner in range(together):
            total_ref[pl.ds(first + inner, rows, stride=stride), :] = total[
                inner * rows : (inner + 1) * rows
            ]

    for stage in (score, attend, finish):
        for group in range(feats // together):
            stage(group)
    result_ref = own[0] if last else out_ref
    for row in range(rows):
        result_ref[row] = total_ref[pl.ds(row * stride, feats), :].astype(jnp.bfloat16)
        if last and (row + 1) % OUT_ROWS == 0:
            first = row + 1 - OUT_ROWS
            send(result_ref.at[pl.ds(first, OUT_ROWS)], first_row + first, OUT_ROWS)
    for copy in copies:
        copy.wait()


OUT_ROWS = 4


def own_rows(parts, feat_qkv, feat_out, item_qkv, item_out, keys, bias, total, first, results):
    feats_here, rows, width = parts[0].shape
    feats = len(parts) * feats_here
    last = first + rows == total
    results = results if last else []
    table = pltpu.VMEM((rows * pitch(feats), width), jnp.float32)
    scratch = [pltpu.VMEM((feats * pitch(rows), width), jnp.float32), table, table, table]
    if last:
        scratch.append(pltpu.VMEM((rows, feats, width), jnp.bfloat16))
        scratch.append(pltpu.SemaphoreType.DMA((len(results) + rows // OUT_ROWS,)))
    block = pl.BlockSpec(memory_space=pltpu.VMEM)
    return pl.pallas_call(
        functools.partial(row_kernel, first, len(results), last),
        out_shape=jax.ShapeDtypeStruct((total if last else rows, feats, width), jnp.bfloat16),
        in_specs=[block] * (len(parts) + 6 + len(results)),
        out_specs=pl.BlockSpec(memory_space=pltpu.HBM) if last else block,
        scratch_shapes=scratch,
        compiler_params=pltpu.CompilerParams(vmem_limit_bytes=24 << 20),
        name="rows",
    )(*parts, feat_qkv, feat_out, item_qkv, item_out, keys, bias, *results)


def swap(tensor, step):
    devices = lax.axis_size("feat")
    return lax.ppermute(tensor, "feat", [(one, one ^ step) for one in range(devices)])


CHUNKS = 2


def one_block_per_table(cells, row_live, row_train, feat_qkv, feat_out, item_qkv, item_out):
    feat_devices = lax.axis_size("feat")
    group_rows = cells.shape[0] // feat_devices
    bias, train_rows, near, sends = prepare(cells, row_live, row_train, CHUNKS)
    near_part = swap(near, 1)
    train_parts = [train_rows, near_part]
    for step in range(2, feat_devices):
        low = step & -step
        if low == step:
            train_parts.append(swap(train_rows, step))
        else:
            train_parts.append(swap(train_parts[step - low], low))
    row_parts = [
        [sends[0][at], near_part]
        + [swap(sends[step][at], step) for step in range(2, feat_devices)]
        for at in range(CHUNKS)
    ]
    keys = key_rows(train_parts, feat_qkv, feat_out, item_qkv)
    results = []
    for at, parts in enumerate(row_parts):
        result = own_rows(
            parts,
            feat_qkv,
            feat_out,
            item_qkv,
            item_out,
            keys,
            bias,
            group_rows,
            at * (group_rows // CHUNKS),
            results,
        )
        results.append(result)
    return results[-1]


def layer(cells, block_table, *rest):
    if block_table.shape[0] == TABLES:
        return one_block_per_table(cells, *rest)
    return on_device(cells, block_table, *rest)


def solution(mesh):
    return jax.shard_map(
        layer,
        mesh=mesh,
        in_specs=(P("rows", "feat", None), P(), P(), P(), P(), P(), P(), P()),
        out_specs=P(("rows", "feat"), None, None),
        check_vma=False,
    )
```

```python
import functools
import math

import jax
import jax.numpy as jnp
from jax import lax
from jax.experimental import pallas as pl
from jax.experimental.pallas import tpu as pltpu
from jax.sharding import PartitionSpec as P

HEADS = 4
HEAD_DIM = 32
KEEP = 4
TABLES = 8


EPSILON = 1e-05
MASKED = -1e30
SCALE2 = HEAD_DIM ** (-0.5) * math.log2(math.e)


def compact_train(train_rows):
    positions = jnp.arange(train_rows.shape[-1], dtype=jnp.int32)
    ordinal = jnp.cumsum(train_rows, axis=-1) - 1
    slot_ids = jnp.arange(KEEP, dtype=jnp.int32)
    matched = (train_rows[..., None, :] == 1) & (ordinal[..., None, :] == slot_ids[:, None])
    return jnp.sum(jnp.where(matched, positions, 0), axis=-1)


def into_heads(tensor):
    return tensor.reshape(tensor.shape[:-1] + (HEADS, HEAD_DIM))


def attend_features(queries, key_part, value_part):
    row_count, query_feats = (queries.shape[0], queries.shape[1])
    blocks = max(1, row_count * query_feats // 1280)
    while row_count % blocks:
        blocks -= 1
    scaling = HEAD_DIM ** (-0.5)

    def attend_one_block(block_parts):
        block_query, block_key, block_value = block_parts
        scores = (
            jnp.einsum(
                "rqhd,rkhd->rhqk", block_query, block_key, preferred_element_type=jnp.float32
            )
            * scaling
        )
        shares = jax.nn.softmax(scores, axis=-1).astype(jnp.bfloat16)
        return jnp.einsum(
            "rhqk,rkhd->rqhd", shares, block_value, preferred_element_type=jnp.float32
        ).astype(jnp.bfloat16)

    def by_block(tensor):
        return tensor.reshape((blocks, row_count // blocks) + tensor.shape[1:])

    result = lax.map(
        attend_one_block, (by_block(queries), by_block(key_part), by_block(value_part))
    )
    return result.reshape(row_count, query_feats, HEADS * HEAD_DIM)


def feature_layer(normed_cells, feat_out, key_part, value_part, queries):
    attended = attend_features(queries, key_part, value_part)
    update = jnp.dot(attended, feat_out, preferred_element_type=jnp.float32)
    return (normed_cells.astype(jnp.float32) + update).astype(jnp.bfloat16)


def on_device(cells, block_table, row_live, row_train, feat_qkv, feat_out, item_qkv, item_out):
    rows_here, _, width_all = cells.shape
    row_index = lax.axis_index("rows")
    feat_index = lax.axis_index("feat")
    row_devices = lax.axis_size("rows")
    feat_devices = lax.axis_size("feat")
    my_table = lax.dynamic_index_in_dim(block_table, row_index, keepdims=False)
    live_rows = lax.dynamic_slice_in_dim(row_live, row_index * rows_here, rows_here).astype(
        jnp.float32
    )
    values = cells.astype(jnp.float32)
    table_hot = (jnp.arange(TABLES, dtype=jnp.int32) == my_table).astype(jnp.float32)
    first_local = jnp.sum(values * live_rows[:, None, None], axis=(0, 2))
    count_local = jnp.sum(live_rows) * width_all
    first_sum, count_sum = lax.psum(
        (table_hot[:, None] * first_local[None, :], table_hot * count_local), "rows"
    )
    table_mean = first_sum / count_sum[:, None]
    mine_mean = lax.dynamic_index_in_dim(table_mean, my_table, keepdims=False)
    centred = values - mine_mean[None, :, None]
    second_local = jnp.sum(centred * centred * live_rows[:, None, None], axis=(0, 2))
    second_sum = lax.psum(table_hot[:, None] * second_local[None, :], "rows")
    table_spread = second_sum / count_sum[:, None]
    mine_spread = lax.dynamic_index_in_dim(table_spread, my_table, keepdims=False)
    normed = (centred * lax.rsqrt(mine_spread + EPSILON)[None, :, None]).astype(jnp.bfloat16)
    normed_rows = lax.all_to_all(normed, "feat", split_axis=0, concat_axis=1, tiled=True)
    projected = jnp.dot(normed_rows, feat_qkv, preferred_element_type=jnp.float32).astype(
        jnp.bfloat16
    )
    queries = into_heads(projected[..., :width_all])
    key_part = into_heads(projected[..., width_all : 2 * width_all])
    value_part = into_heads(projected[..., 2 * width_all :])
    mixed_rows = feature_layer(normed_rows, feat_out, key_part, value_part, queries)
    group_rows, total_feats = (mixed_rows.shape[0], mixed_rows.shape[1])
    per_device = total_feats * HEADS // row_devices
    first_row = row_index * rows_here + feat_index * group_rows
    train_here = lax.dynamic_slice_in_dim(row_train, first_row, group_rows)
    places = compact_train(train_here)
    chosen = jnp.take(mixed_rows, places, axis=0)
    item_query = jnp.dot(
        mixed_rows, item_qkv[:, :width_all], preferred_element_type=jnp.float32
    ).astype(jnp.bfloat16)
    item_query = item_query.reshape(group_rows, row_devices, per_device, HEAD_DIM)
    key_value = jnp.dot(chosen, item_qkv[:, width_all:], preferred_element_type=jnp.float32).astype(
        jnp.bfloat16
    )
    item_key = key_value[..., :width_all].reshape(KEEP, row_devices, per_device, HEAD_DIM)
    item_value = key_value[..., width_all:].reshape(KEEP, row_devices, per_device, HEAD_DIM)
    query_table = jnp.repeat(block_table, group_rows)
    groups_all = row_train.reshape(row_devices, feat_devices, group_rows)
    group_counts = jnp.sum(groups_all, axis=2)
    slot_ids = jnp.arange(KEEP, dtype=jnp.int32)
    key_valid = slot_ids[None, None, :] < jnp.transpose(group_counts)[:, :, None]
    key_table = jnp.broadcast_to(block_table[None, :, None], key_valid.shape)
    allowed = (query_table[:, None] == key_table.reshape(-1)[None, :]) & key_valid.reshape(-1)[
        None, :
    ]
    query_count = query_table.shape[0]
    key_count = allowed.shape[1]
    query_blocks = max(1, query_count // 512)
    while query_count % query_blocks:
        query_blocks -= 1
    scaling = HEAD_DIM ** (-0.5)
    blocked_allowed = allowed.reshape(query_blocks, query_count // query_blocks, key_count)
    local_query = lax.all_to_all(item_query, "rows", split_axis=1, concat_axis=0, tiled=True)
    local_key = lax.all_to_all(item_key, "rows", split_axis=1, concat_axis=0, tiled=True)
    local_value = lax.all_to_all(item_value, "rows", split_axis=1, concat_axis=0, tiled=True)
    every_key = lax.all_gather(local_key, "feat", axis=0, tiled=True)
    every_value = lax.all_gather(local_value, "feat", axis=0, tiled=True)

    def one_item(item_parts):
        single_query, single_key, single_value = item_parts

        def one_one_block(block_parts):
            block_query, block_allowed = block_parts
            scores = (
                jnp.dot(block_query, single_key.T, preferred_element_type=jnp.float32) * scaling
            )
            scores = jnp.where(block_allowed, scores, MASKED)
            shares = jax.nn.softmax(scores, axis=-1).astype(jnp.bfloat16)
            return jnp.dot(shares, single_value, preferred_element_type=jnp.float32).astype(
                jnp.bfloat16
            )

        blocked_query = single_query.reshape(query_blocks, query_count // query_blocks, HEAD_DIM)
        return lax.map(one_one_block, (blocked_query, blocked_allowed)).reshape(
            query_count, HEAD_DIM
        )

    by_item = (
        jnp.moveaxis(local_query[:, 0], 1, 0),
        jnp.moveaxis(every_key[:, 0], 1, 0),
        jnp.moveaxis(every_value[:, 0], 1, 0),
    )
    result = jnp.moveaxis(lax.map(one_item, by_item), 0, 1)[:, None]
    attended = lax.all_to_all(result, "rows", split_axis=0, concat_axis=1, tiled=True)
    attended = attended.reshape(group_rows, total_feats, width_all)
    update = jnp.dot(attended, item_out, preferred_element_type=jnp.float32)
    return (mixed_rows.astype(jnp.float32) + update).astype(jnp.bfloat16)


def vmem_kernel(body, shapes, count, scratch, limit):
    many = isinstance(shapes, list)
    block = pl.BlockSpec(memory_space=pltpu.VMEM)
    return pl.pallas_call(
        body,
        out_shape=shapes,
        in_specs=[block] * count,
        out_specs=[block] * len(shapes) if many else block,
        scratch_shapes=scratch,
        compiler_params=pltpu.CompilerParams(vmem_limit_bytes=limit << 20),
    )


PIECES = 1


def prepare_kernel(chunks, live_in, train_in, cells_in, bias_ref, train_out, *refs):
    outs, (live_ref, train_ref, cells_ref, sems) = refs[:-4], refs[-4:]
    feats_here, rows_here, width = cells_ref.shape
    feat_devices = lax.axis_size("feat")
    group_rows = rows_here // feat_devices
    feat_index = lax.axis_index("feat")
    row_index = lax.axis_index("rows")
    keys = train_out.shape[1]
    piece = feats_here // math.gcd(feats_here, PIECES)

    copies = [
        pltpu.make_async_copy(live_in, live_ref, sems.at[0]),
        pltpu.make_async_copy(train_in, train_ref, sems.at[1]),
    ]
    for at, feat in enumerate(range(0, feats_here, piece)):
        here = pl.ds(feat, piece)
        copies.append(
            pltpu.make_async_copy(cells_in.at[here], cells_ref.at[here], sems.at[2 + at])
        )
    for copy in copies:
        copy.start()
    for copy in copies[:2]:
        copy.wait()

    live = live_ref[pl.ds(row_index, 1), :].astype(jnp.float32)
    count = jnp.sum(live, axis=1, keepdims=True) * width
    weight = jnp.transpose(jnp.broadcast_to(live, (width, rows_here)))

    train = jnp.broadcast_to(train_ref[pl.ds(row_index, 1), :], (keys, rows_here))
    before = lax.broadcasted_iota(jnp.int32, (rows_here, rows_here), 0)
    after = lax.broadcasted_iota(jnp.int32, (rows_here, rows_here), 1)
    ladder = (before <= after) & (before // group_rows == after // group_rows)
    ordinal = jnp.dot(
        train.astype(jnp.float32).astype(jnp.bfloat16),
        jnp.where(ladder, 1.0, 0.0).astype(jnp.bfloat16),
        preferred_element_type=jnp.float32,
    )
    key = lax.broadcasted_iota(jnp.int32, (keys, rows_here), 0)
    row = lax.broadcasted_iota(jnp.int32, (keys, rows_here), 1)
    here = (
        (train == 1)
        & (row // group_rows == key // KEEP)
        & (ordinal == (key % KEEP + 1).astype(jnp.float32))
    )
    chosen = jnp.where(here, 1.0, 0.0)
    found = jnp.sum(chosen, axis=1, keepdims=True)
    bias_ref[...] = jnp.broadcast_to(jnp.where(found > 0.5, 0.0, MASKED), bias_ref.shape)
    picks = jnp.concatenate(
        [chosen, jnp.broadcast_to(live, (keys, rows_here))], axis=0
    ).astype(jnp.bfloat16)

    means, train_rows = [], []
    for feat in range(feats_here):
        if feat % piece == 0:
            copies[2 + feat // piece].wait()
        picked = jnp.dot(picks, cells_ref[feat], preferred_element_type=jnp.float32)
        train_rows.append(picked[:keys])
        total = jnp.sum(picked[keys : keys + 1], axis=1, keepdims=True)
        means.append(jnp.broadcast_to(total / count, (1, width)))
    factors = []
    for feat in range(feats_here):
        centred = cells_ref[feat].astype(jnp.float32) - means[feat]
        total = jnp.sum(centred * centred * weight, axis=0, keepdims=True)
        spread = jnp.sum(total, axis=1, keepdims=True) / count
        factors.append(jnp.broadcast_to(lax.rsqrt(spread + EPSILON), (1, width)))

    def normed(feat, values):
        centred = values.astype(jnp.float32) - means[feat]
        return (centred * factors[feat]).astype(jnp.bfloat16)

    near_out = outs[0]
    for feat in range(feats_here):
        rows = normed(feat, train_rows[feat])
        train_out[feat] = rows
        near_out[0, feat] = rows
    for step in range(feat_devices):
        for at in range(chunks):
            size = group_rows // chunks
            first_row = pl.multiple_of((feat_index ^ step) * group_rows + at * size, size)
            for feat in range(feats_here):
                rows = normed(feat, cells_ref[feat, pl.ds(first_row, size), :])
                if step == 1:
                    near_out[1 + at, feat] = rows
                else:
                    outs[1 + max(step - 1, 0) * chunks + at][feat] = rows


def prepare(cells, row_live, row_train, chunks):
    rows_here, feats_here, width = cells.shape
    feat_devices = lax.axis_size("feat")
    keys = feat_devices * KEEP
    shapes = [
        jax.ShapeDtypeStruct((keys, 128), jnp.float32),
        jax.ShapeDtypeStruct((feats_here, keys, width), jnp.bfloat16),
    ]
    size = rows_here // feat_devices // chunks
    assert size == keys
    part = jax.ShapeDtypeStruct((feats_here, size, width), jnp.bfloat16)
    shapes.append(jax.ShapeDtypeStruct((1 + chunks,) + part.shape, jnp.bfloat16))
    shapes += [part] * ((feat_devices - 1) * chunks)
    blocks = row_live.shape[0] // rows_here
    block = pl.BlockSpec(memory_space=pltpu.VMEM)
    outs = pl.pallas_call(
        functools.partial(prepare_kernel, chunks),
        out_shape=shapes,
        in_specs=[pl.BlockSpec(memory_space=pltpu.HBM)] * 3,
        out_specs=[block] * len(shapes),
        scratch_shapes=[
            pltpu.VMEM((blocks, rows_here), jnp.int32),
            pltpu.VMEM((blocks, rows_here), jnp.int32),
            pltpu.VMEM((feats_here, rows_here, width), jnp.bfloat16),
            pltpu.SemaphoreType.DMA((2 + math.gcd(feats_here, PIECES),)),
        ],
        compiler_params=pltpu.CompilerParams(vmem_limit_bytes=8 << 20),
        name="prepare",
    )(
        pltpu.with_memory_space_constraint(row_live.reshape(-1, rows_here), pltpu.HBM),
        pltpu.with_memory_space_constraint(row_train.reshape(-1, rows_here), pltpu.HBM),
        pltpu.with_memory_space_constraint(jnp.transpose(cells, (1, 0, 2)), pltpu.HBM),
    )
    sends = {
        step: outs[3 + at * chunks : 3 + (at + 1) * chunks]
        for at, step in enumerate([0, *range(2, feat_devices)])
    }
    return outs[0], outs[1], outs[2], sends


def pitch(count):
    return count + 4 if count % 8 == 0 else count


def gather_parts(parts, at, held):
    feat_index = lax.axis_index("feat")
    feats_here, rows, _ = parts[0].shape
    for step, part in enumerate(parts):
        first = (feat_index ^ step) * (feats_here * pitch(rows))
        values = part[at] if step == 1 else part[...]
        for feat in range(feats_here):
            held[pl.ds(first + feat * pitch(rows), rows), :] = values[feat].astype(jnp.float32)


def head_masks(rows, width):
    lane = lax.broadcasted_iota(jnp.int32, (rows, width), 1)
    return [(lane // HEAD_DIM) == head for head in range(HEADS)]


def by_head(tensor, masks):
    return [jnp.where(mask, tensor, jnp.zeros_like(tensor)) for mask in masks]


def staggered(stages, count, lag=1):
    for step in range(count + lag * (len(stages) - 1)):
        for at, stage in enumerate(stages):
            if 0 <= step - at * lag < count:
                stage(step - at * lag)


def over_keys(scores, axis):
    top = jnp.max(scores, axis=axis, keepdims=True)
    powers = jnp.exp2(scores - top)
    return powers * (1.0 / jnp.sum(powers, axis=axis, keepdims=True))


def feature_shares(queries, keys, masks):
    count = queries.shape[0]
    scores = lax.dot_general(
        jnp.concatenate(by_head(keys, masks), axis=0),
        queries,
        (((1,), (1,)), ((), ())),
        preferred_element_type=jnp.float32,
    ).reshape(HEADS, count, count)
    return over_keys(scores, 1).reshape(HEADS * count, count).astype(jnp.bfloat16)


def feature_values(shares, values, masks):
    return lax.dot_general(
        shares,
        jnp.concatenate(by_head(values, masks), axis=0),
        (((0,), (0,)), ((), ())),
        preferred_element_type=jnp.float32,
    ).astype(jnp.bfloat16)


STEP = 4


def feature_rows(held, rows, qkv_ref, out_ref, consume):
    feats, width = held.shape[0] // pitch(rows), held.shape[1]
    masks = head_masks(feats, width)
    size = math.gcd(rows, STEP)
    cells, projected, shares, attended = {}, {}, {}, {}

    def project(group):
        cells[group] = jnp.concatenate(
            [
                held[pl.ds(group * size + row, feats, stride=pitch(rows)), :]
                for row in range(size)
            ],
            axis=0,
        )
        every = jnp.dot(
            cells[group].astype(jnp.bfloat16), qkv_ref[...], preferred_element_type=jnp.float32
        )
        projected[group] = [
            (every[:, :width] * SCALE2).astype(jnp.bfloat16),
            every[:, width : 2 * width].astype(jnp.bfloat16),
            every[:, 2 * width :].astype(jnp.bfloat16),
        ]

    def score(group):
        queries, keys, _ = projected[group]
        shares[group] = [
            feature_shares(
                queries[row * feats : (row + 1) * feats],
                keys[row * feats : (row + 1) * feats],
                masks,
            )
            for row in range(size)
        ]

    def attend(group):
        values = projected.pop(group)[2]
        attended[group] = jnp.concatenate(
            [
                feature_values(part, values[row * feats : (row + 1) * feats], masks)
                for row, part in enumerate(shares.pop(group))
            ],
            axis=0,
        )

    def mix(group):
        update = jnp.dot(
            attended.pop(group), out_ref[...], preferred_element_type=jnp.float32
        )
        consume(group * size, size, (cells.pop(group) + update).astype(jnp.bfloat16))

    staggered([project, score, attend, mix], rows // size, 1)


def put_rows(table, first, count, values):
    feats = values.shape[0] // count
    for row in range(count):
        table[pl.ds((first + row) * pitch(feats), feats), :] = values[
            row * feats : (row + 1) * feats
        ]


def by_feature(mixed_ref, first, count, rows, stride):
    return jnp.concatenate(
        [mixed_ref[pl.ds(first + feat, rows, stride=stride), :] for feat in range(count)], axis=0
    )


def key_kernel(*refs):
    feat_devices = lax.axis_size("feat")
    parts = refs[:feat_devices]
    feat_qkv, feat_out, item_qkv, key_ref, value_ref, held = refs[feat_devices:]
    rows, width = parts[0].shape[1], held.shape[1]
    gather_parts(parts, 0, held)

    def consume(first, count, mixed):
        both = jnp.dot(mixed, item_qkv[:, width:], preferred_element_type=jnp.float32)
        put_rows(key_ref, first, count, both[:, :width])
        put_rows(value_ref, first, count, both[:, width:])

    feature_rows(held, rows, feat_qkv, feat_out, consume)


def key_rows(parts, feat_qkv, feat_out, item_qkv):
    feats_here, rows, width = parts[0].shape
    feats = len(parts) * feats_here
    table = jax.ShapeDtypeStruct((rows * pitch(feats), width), jnp.float32)
    return vmem_kernel(
        key_kernel,
        [table, table],
        len(parts) + 3,
        [pltpu.VMEM((feats * pitch(rows), width), jnp.float32)],
        24,
    )(*parts, feat_qkv, feat_out, item_qkv)


def row_kernel(first_row, earlier, last, *refs):
    feat_devices = lax.axis_size("feat")
    parts = refs[:feat_devices]
    (feat_qkv, feat_out, item_qkv, item_out, key_ref, value_ref, bias_ref) = refs[
        feat_devices : feat_devices + 7
    ]
    results = refs[feat_devices + 7 : feat_devices + 7 + earlier]
    out_ref, held, mixed_ref, query_ref, total_ref, *own = refs[
        feat_devices + 7 + earlier :
    ]
    rows, width = parts[0].shape[1], held.shape[1]
    feats, keys = feat_devices * parts[0].shape[0], bias_ref.shape[0]
    copies = []

    def send(source, at, count):
        copy = pltpu.make_async_copy(source, out_ref.at[pl.ds(at, count)], own[1].at[len(copies)])
        copy.start()
        copies.append(copy)

    for at, result in enumerate(results):
        send(result, at * rows, rows)
    gather_parts(parts, 1 + first_row // rows, held)

    def consume(first, count, mixed):
        put_rows(mixed_ref, first, count, mixed.astype(jnp.float32))
        queries = jnp.dot(mixed, item_qkv[:, :width], preferred_element_type=jnp.float32)
        put_rows(query_ref, first, count, queries * SCALE2)

    feature_rows(held, rows, feat_qkv, feat_out, consume)

    stride = pitch(feats)
    together = 128 // rows
    lanes = together * rows
    size = HEADS * keys
    key_masks = head_masks(keys, width)
    bias = jnp.concatenate([bias_ref[:, :lanes]] * HEADS, axis=0)
    lane_owner = lax.broadcasted_iota(jnp.int32, (size, lanes), 1) // rows
    pair_row = lax.broadcasted_iota(jnp.int32, (2 * rows, 2 * size), 0) // rows
    pair_lane = lax.broadcasted_iota(jnp.int32, (2 * rows, 2 * size), 1) // size
    pair_mask = pair_row == pair_lane

    shares, attended = {}, {}

    def score(group):
        first = group * together
        stacked_keys = []
        for feat in range(first, first + together):
            stacked_keys += by_head(
                key_ref[pl.ds(feat, keys, stride=stride), :].astype(jnp.bfloat16), key_masks
            )
        every = lax.dot_general(
            jnp.concatenate(stacked_keys, axis=0),
            by_feature(query_ref, first, together, rows, stride).astype(jnp.bfloat16),
            (((1,), (1,)), ((), ())),
            preferred_element_type=jnp.float32,
        )
        scores = every[:size]
        for inner in range(1, together):
            scores = jnp.where(lane_owner == inner, every[inner * size : (inner + 1) * size], scores)
        part = over_keys((scores + bias).reshape(HEADS, keys, lanes), 1).reshape(size, lanes)
        shares[group] = jnp.transpose(jnp.concatenate([part, part], axis=0)).astype(jnp.bfloat16)

    def attend(group):
        part, results = shares.pop(group), []
        for pair in range(together // 2):
            block = part[pair * 2 * rows : (pair + 1) * 2 * rows]
            stacked_values = []
            for inner in range(2):
                feat = group * together + pair * 2 + inner
                stacked_values += by_head(
                    value_ref[pl.ds(feat, keys, stride=stride), :].astype(jnp.bfloat16), key_masks
                )
            results.append(
                jnp.dot(
                    jnp.where(pair_mask, block, jnp.zeros_like(block)),
                    jnp.concatenate(stacked_values, axis=0),
                    preferred_element_type=jnp.float32,
                ).astype(jnp.bfloat16)
            )
        attended[group] = jnp.concatenate(results, axis=0)

    def finish(group):
        first = group * together
        update = jnp.dot(attended.pop(group), item_out[...], preferred_element_type=jnp.float32)
        total = by_feature(mixed_ref, first, together, rows, stride) + update
        for inner in range(together):
            total_ref[pl.ds(first + inner, rows, stride=stride), :] = total[
                inner * rows : (inner + 1) * rows
            ]

    for stage in (score, attend, finish):
        for group in range(feats // together):
            stage(group)
    result_ref = own[0] if last else out_ref
    for row in range(rows):
        result_ref[row] = total_ref[pl.ds(row * stride, feats), :].astype(jnp.bfloat16)
        if last and (row + 1) % OUT_ROWS == 0:
            first = row + 1 - OUT_ROWS
            send(result_ref.at[pl.ds(first, OUT_ROWS)], first_row + first, OUT_ROWS)
    for copy in copies:
        copy.wait()


OUT_ROWS = 4


def own_rows(parts, feat_qkv, feat_out, item_qkv, item_out, keys, bias, total, first, results):
    feats_here, rows, width = parts[0].shape
    feats = len(parts) * feats_here
    last = first + rows == total
    results = results if last else []
    table = pltpu.VMEM((rows * pitch(feats), width), jnp.float32)
    scratch = [pltpu.VMEM((feats * pitch(rows), width), jnp.float32), table, table, table]
    if last:
        scratch.append(pltpu.VMEM((rows, feats, width), jnp.bfloat16))
        scratch.append(pltpu.SemaphoreType.DMA((len(results) + rows // OUT_ROWS,)))
    block = pl.BlockSpec(memory_space=pltpu.VMEM)
    return pl.pallas_call(
        functools.partial(row_kernel, first, len(results), last),
        out_shape=jax.ShapeDtypeStruct((total if last else rows, feats, width), jnp.bfloat16),
        in_specs=[block] * (len(parts) + 7 + len(results)),
        out_specs=pl.BlockSpec(memory_space=pltpu.HBM) if last else block,
        scratch_shapes=scratch,
        compiler_params=pltpu.CompilerParams(vmem_limit_bytes=24 << 20),
        name="rows",
    )(*parts, feat_qkv, feat_out, item_qkv, item_out, *keys, bias, *results)


def swap(tensor, step):
    devices = lax.axis_size("feat")
    return lax.ppermute(tensor, "feat", [(one, one ^ step) for one in range(devices)])


CHUNKS = 2


def one_block_per_table(cells, row_live, row_train, feat_qkv, feat_out, item_qkv, item_out):
    feat_devices = lax.axis_size("feat")
    group_rows = cells.shape[0] // feat_devices
    bias, train_rows, near, sends = prepare(cells, row_live, row_train, CHUNKS)
    near_part = swap(near, 1)
    train_parts = [train_rows, near_part]
    for step in range(2, feat_devices):
        low = step & -step
        if low == step:
            train_parts.append(swap(train_rows, step))
        else:
            train_parts.append(swap(train_parts[step - low], low))
    row_parts = [
        [sends[0][at], near_part]
        + [swap(sends[step][at], step) for step in range(2, feat_devices)]
        for at in range(CHUNKS)
    ]
    keys = key_rows(train_parts, feat_qkv, feat_out, item_qkv)
    results = []
    for at, parts in enumerate(row_parts):
        result = own_rows(
            parts,
            feat_qkv,
            feat_out,
            item_qkv,
            item_out,
            keys,
            bias,
            group_rows,
            at * (group_rows // CHUNKS),
            results,
        )
        results.append(result)
    return results[-1]


def layer(cells, block_table, *rest):
    if block_table.shape[0] == TABLES:
        return one_block_per_table(cells, *rest)
    return on_device(cells, block_table, *rest)


def solution(mesh):
    return jax.shard_map(
        layer,
        mesh=mesh,
        in_specs=(P("rows", "feat", None), P(), P(), P(), P(), P(), P(), P()),
        out_specs=P(("rows", "feat"), None, None),
        check_vma=False,
    )
```
